32 devices in a mesh: gx: 8 (over z, y), gy: 4 (over x, core).
Axes of the slice: x: 2, y: 2, z: 4, core: 2. Of those that a mesh axis runs over, the one named last changes fastest.
Arguments:
- charge_density: float32 [256, 256, 256], P('gx', 'gy'), may hold values from -5080 to 5140
Outputs:
- potential: float32 [256, 256, 256], P('gx', 'gy')
- energies: float32 [2], replicated
The draws below stay inside these ranges and needn't reach their ends.
All inputs are finite; a program needn't handle non-finite values.
Results may differ from the reference program's by a relative error of at most 0.0003.
Values sent between devices are 32-bit elements.
No kernel may reach another device: no remote copies, remote signals or barrier semaphores. Data moves between devices by JAX's collectives and lax.ppermute only.
A program may use at most 192 MiB of HBM per device.

```python
import math
import jax
import jax.numpy as jnp
import numpy as np
from jax import lax

N = 256
ORDER = 16


def draw_charge_density(key, part):
    level_key, noise_key = jax.random.split(jax.random.fold_in(key, 11))
    bound = float((N + 1) * (N + 1) // 13)
    levels = jax.random.uniform(level_key, (8, 8, 8), jnp.float32, minval=0.0, maxval=60.0)
    noise = jax.random.uniform(noise_key, (N, N, N), jnp.float32, minval=-bound, maxval=bound)
    block = N // 8
    coarse = jnp.repeat(jnp.repeat(jnp.repeat(levels, block, 0), block, 1), block, 2)
    return (coarse + noise).astype(jnp.float32)


def setup_inputs(seed: int = 0) -> dict:
    key_of = jax.random.split(jax.random.key(seed), 2)
    return {
        "charge_density": draw_charge_density(jax.random.fold_in(key_of[1], 71), 0),
    }


exact_mode = lax.Precision.HIGHEST
outer_ratio = 1.1
radius_scale = math.sqrt(3.0) / 2.0

def sine_table(length):
    counter = jnp.arange(length, dtype=jnp.int32) + 1
    product = counter[:, None] * counter[None, :] % (2 * (length + 1))
    return jnp.sin(math.pi * product.astype(jnp.float32) / (length + 1))

def eigen_line(counter, length):
    half_angle = math.pi * (counter + 1).astype(jnp.float32) / (2.0 * (length + 1))
    return 4.0 * float((length + 1) * (length + 1)) * jnp.sin(half_angle) ** 2

def recurrence_tables():
    degree_count = ORDER + 1
    near_coeff = np.zeros((degree_count, degree_count, 1), np.float32)
    far_coeff = np.zeros((degree_count, degree_count, 1), np.float32)
    sector = np.ones(degree_count, np.float32)
    for degree in range(1, degree_count):
        for azimuth in range(degree):
            divisor = math.sqrt(degree * degree - azimuth * azimuth)
            near_coeff[degree, azimuth, 0] = (2 * degree - 1) / divisor
            far_coeff[degree, azimuth, 0] = math.sqrt((degree - 1) * (degree - 1) - azimuth * azimuth) / divisor
        if degree >= 2:
            sector[degree] = math.sqrt((2 * degree - 1) / (2.0 * degree))
    return (near_coeff, far_coeff, sector)

def expansion_weights():
    degree_count = ORDER + 1
    weights = np.zeros((degree_count, degree_count), np.float32)
    for degree in range(degree_count):
        for azimuth in range(degree + 1):
            factor = 1.0 if azimuth == 0 else 2.0
            weights[degree, azimuth] = factor / (4.0 * math.pi * radius_scale * outer_ratio ** (degree + 1))
    return weights

def harmonic_sweep(unit_x, unit_y, unit_z, visitor, running):
    near_coeff, far_coeff, sector = recurrence_tables()
    degree_count = ORDER + 1
    selector = np.eye(degree_count, dtype=np.float32)[:, :, None]
    empty_rows = jnp.zeros((degree_count,) + unit_x.shape, unit_x.dtype)
    sector_cosine = jnp.ones_like(unit_x)
    sector_sine = jnp.zeros_like(unit_x)
    cosine_prev, sine_prev, cosine_old, sine_old = (empty_rows, empty_rows, empty_rows, empty_rows)
    for degree in range(degree_count):
        if degree > 0:
            sector_cosine, sector_sine = (sector[degree] * (unit_x * sector_cosine - unit_y * sector_sine), sector[degree] * (unit_x * sector_sine + unit_y * sector_cosine))
        cosine_now = near_coeff[degree] * unit_z * cosine_prev - far_coeff[degree] * cosine_old + selector[degree] * sector_cosine
        sine_now = near_coeff[degree] * unit_z * sine_prev - far_coeff[degree] * sine_old + selector[degree] * sector_sine
        running = visitor(running, degree, cosine_now, sine_now)
        cosine_old, sine_old = (cosine_prev, sine_prev)
        cosine_prev, sine_prev = (cosine_now, sine_now)
    return running

def face_moments(point_x, point_y, point_z, charge):
    radius = jnp.sqrt(point_x * point_x + point_y * point_y + point_z * point_z)
    scaled_radius = radius / radius_scale

    def visitor(running, degree, cosine_now, sine_now):
        weight, moment_cosine, moment_sine, facing_cosine, facing_sine = running
        moment_cosine = moment_cosine + [jnp.dot(cosine_now, weight, precision=exact_mode)]
        moment_sine = moment_sine + [jnp.dot(sine_now, weight, precision=exact_mode)]
        facing_cosine = facing_cosine + [jnp.dot(cosine_now, charge, precision=exact_mode)]
        facing_sine = facing_sine + [jnp.dot(sine_now, charge, precision=exact_mode)]
        return (weight * scaled_radius, moment_cosine, moment_sine, facing_cosine, facing_sine)
    result = harmonic_sweep(point_x / radius, point_y / radius, point_z / radius, visitor, (charge, [], [], [], []))
    return tuple((jnp.stack(listing) for listing in result[1:]))

def face_potential(point_x, point_y, point_z, weight_cosine, weight_sine):
    radius = jnp.sqrt(point_x * point_x + point_y * point_y + point_z * point_z)

    def visitor(accum, degree, cosine_now, sine_now):
        accum = accum + jnp.dot(weight_cosine[degree], cosine_now, precision=exact_mode)
        return accum + jnp.dot(weight_sine[degree], sine_now, precision=exact_mode)
    return harmonic_sweep(point_x / radius, point_y / radius, point_z / radius, visitor, jnp.zeros_like(point_x))

def transform(volume, sine_rows):
    volume = jnp.einsum('abc,ck->abk', volume, sine_rows, precision=exact_mode)
    volume = jnp.einsum('abk,bj->ajk', volume, sine_rows, precision=exact_mode)
    return jnp.einsum('ajk,ai->ijk', volume, sine_rows, precision=exact_mode)

def poisson_solve(volume, sine_rows, denominator):
    return transform(transform(volume, sine_rows) / denominator, sine_rows)

def reference(charge_density):
    length = N
    spacing = 1.0 / (length + 1)
    sine_rows = sine_table(length)
    eigen_rows = eigen_line(jnp.arange(length, dtype=jnp.int32), length)
    denominator = (eigen_rows[:, None, None] + eigen_rows[None, :, None] + eigen_rows[None, None, :]) * ((length + 1) / 2.0) ** 3
    first_field = poisson_solve(charge_density, sine_rows, denominator)
    coords = (jnp.arange(length, dtype=jnp.float32) - (length - 1) / 2.0) * spacing
    grid_rows = jnp.broadcast_to(coords[:, None], (length, length)).reshape(-1)
    grid_columns = jnp.broadcast_to(coords[None, :], (length, length)).reshape(-1)
    plane_half = jnp.full((length * length,), 0.5, jnp.float32)
    boundary_faces = [(grid_rows, grid_columns, -plane_half, first_field[:, :, 0]), (grid_rows, grid_columns, plane_half, first_field[:, :, -1]), (-plane_half, grid_rows, grid_columns, first_field[0]), (plane_half, grid_rows, grid_columns, first_field[-1]), (grid_rows, -plane_half, grid_columns, first_field[:, 0]), (grid_rows, plane_half, grid_columns, first_field[:, -1])]
    totals = None
    for point_x, point_y, point_z, near_cells in boundary_faces:
        face_terms = face_moments(point_x, point_y, point_z, spacing * near_cells.reshape(-1))
        if totals is None:
            totals = face_terms
        else:
            totals = tuple((earlier + later for earlier, later in zip(totals, face_terms)))
    weights = expansion_weights()
    weight_cosine = weights * totals[0]
    weight_sine = weights * totals[1]
    potentials = []
    for point_x, point_y, point_z, near_cells in boundary_faces:
        potentials.append(face_potential(point_x, point_y, point_z, weight_cosine, weight_sine).reshape(length, length) / spacing ** 2)
    source = charge_density
    source = source.at[:, :, 0].add(potentials[0])
    source = source.at[:, :, -1].add(potentials[1])
    source = source.at[0].add(potentials[2])
    source = source.at[-1].add(potentials[3])
    source = source.at[:, 0].add(potentials[4])
    source = source.at[:, -1].add(potentials[5])
    potential = poisson_solve(source, sine_rows, denominator)
    energies = spacing ** 3 * jnp.stack([jnp.sum(charge_density * first_field), jnp.sum(charge_density * potential)])
    return (potential, energies)
```

```python
import functools
import math

import jax
import jax.numpy as jnp
import numpy as np
from jax import lax
from jax.experimental import pallas as pl
from jax.experimental.pallas import tpu as pltpu
from jax.sharding import PartitionSpec as P

ORDER = 16
COUNT = ORDER + 1
PAIRS = 384
TERMS = 384
outer_ratio = 1.1
radius_scale = math.sqrt(3.0) / 2.0
F32 = jnp.float32
BF16 = jnp.bfloat16
EXACT = lax.Precision.HIGHEST


NN = (((1,), (0,)), ((), ()))
NT = (((1,), (1,)), ((), ()))
TN = (((0,), (0,)), ((), ()))


def term_list():
    terms = [(0, l, m) for m in range(COUNT) for l in range(m, COUNT)]
    terms += [(1, l, m) for m in range(1, COUNT) for l in range(m, COUNT)]
    return terms


def split_np(table):
    import ml_dtypes

    high = table.astype(np.float32).astype(ml_dtypes.bfloat16)
    low = (table - high.astype(np.float64)).astype(np.float32).astype(ml_dtypes.bfloat16)
    return high, low


def split(value):
    high = value.astype(BF16)
    return high, (value - high.astype(F32)).astype(BF16)


def mul(left, right, dims):
    return lax.dot_general(left, right, dims, preferred_element_type=F32)


def exact(left, right, dims):
    return lax.dot_general(left, right, dims, precision=EXACT, preferred_element_type=F32)


def solid_values(x, y, z):
    squared = x * x + y * y + z * z
    cosine, sine = {}, {}
    cosine[0, 0], sine[0, 0] = np.ones_like(x), np.zeros_like(x)
    for l in range(1, COUNT):
        scale = math.sqrt((2 * l - 1) / (2.0 * l)) if l > 1 else 1.0
        cosine[l, l] = scale * (x * cosine[l - 1, l - 1] - y * sine[l - 1, l - 1])
        sine[l, l] = scale * (x * sine[l - 1, l - 1] + y * cosine[l - 1, l - 1])
    for table in (cosine, sine):
        for m in range(COUNT):
            for l in range(m + 1, COUNT):
                older = table[l - 2, m] if l - 2 >= m else np.zeros_like(x)
                table[l, m] = (
                    (2 * l - 1) * z * table[l - 1, m]
                    - math.sqrt((l - 1) ** 2 - m * m) * squared * older
                ) / math.sqrt(l * l - m * m)
    return [(cosine, sine)[kind][l, m] for kind, l, m in term_list()]


@functools.cache
def constants(length):
    step = length + 1
    index = np.arange(length) + 1
    sine = np.sin(np.pi * ((index[:, None] * index[None, :]) % (2 * step)) / step)
    eigen = 4.0 * np.sin(np.pi * index / (2.0 * step)) ** 2
    cells = (np.arange(length) - (length - 1) / 2.0) / step
    legendre = np.stack(
        [np.polynomial.legendre.legval(2 * cells, np.eye(COUNT)[p]) for p in range(COUNT)]
    )
    hat = legendre @ sine
    slow = np.zeros((length, PAIRS))
    fast = np.zeros((length, PAIRS))
    for first in range(COUNT):
        for second in range(COUNT):
            slow[:, first * COUNT + second] = hat[first]
            fast[:, first * COUNT + second] = hat[second]
    edges = np.stack([sine[0] + sine[-1], sine[-1] - sine[0]])
    nodes, weights = np.polynomial.legendre.leggauss(COUNT + 3)
    basis = np.stack([np.polynomial.legendre.legval(nodes, np.eye(COUNT)[p]) for p in range(COUNT)])
    project = basis * weights[None, :] * (2 * np.arange(COUNT)[:, None] + 1) / 2.0
    first, second = np.meshgrid(nodes / 2.0, nodes / 2.0, indexing="ij")
    half = np.full_like(first, 0.5)
    terms = term_list()
    scale = (1.0 / step) * (2.0 / step) ** 2
    maps = np.zeros((3, PAIRS, TERMS))
    places = [(half, first, second), (first, half, second), (first, second, half)]
    for face, place in enumerate(places):
        for column, values in enumerate(solid_values(*place)):
            degree = terms[column][1]
            expansion = project @ values @ project.T
            maps[face, : COUNT * COUNT, column] = (
                scale * expansion.reshape(-1) / radius_scale**degree
            )
    masks = np.zeros((3, 8, TERMS))
    for column, (kind, l, m) in enumerate(terms):
        masks[0, (m + kind) % 2, column] = 1.0
        masks[1, kind, column] = 1.0
        masks[2, (l - m) % 2, column] = 1.0
    folded = np.zeros((2, length // 2, length))
    parity = np.arange(length) % 2
    upper = 2.0 * sine[length // 2 :]
    folded[0] = upper * (parity == 0)
    folded[1] = upper * (parity == 1)
    return dict(
        sine=sine,
        eigen=eigen,
        cells=cells,
        legendre=legendre,
        slow=slow,
        fast=fast,
        edges=edges,
        maps=maps,
        masks=masks,
        folded=folded.reshape(length, length),
    )


def evaluation_scales():
    sector, running = [1.0], 1.0
    for l in range(1, COUNT):
        running *= math.sqrt((2 * l - 1) / (2.0 * l)) if l > 1 else 1.0
        sector.append(running)
    kappa, beta = {}, {}
    for m in range(COUNT):
        kappa[m, m] = sector[m]
        previous = 1.0
        for l in range(m + 1, COUNT):
            near = (2 * l - 1) / math.sqrt(l * l - m * m)
            far = math.sqrt((l - 1) ** 2 - m * m) / math.sqrt(l * l - m * m)
            kappa[l, m] = kappa[l - 1, m] * near
            beta[l, m] = far / (near * previous) if l >= m + 2 else 0.0
            previous = near
    scales = np.zeros((TERMS, 128))
    for row, (_, l, m) in enumerate(term_list()):
        factor = 1.0 if m == 0 else 2.0
        weight = factor / (4.0 * math.pi * radius_scale * outer_ratio ** (l + 1))
        scales[row, :] = weight * kappa[l, m]
    return scales, beta


def evaluate(coef, unit_x, unit_y, unit_z, keep_azimuth):
    beta = evaluation_scales()[1]
    rows = {term: row for row, term in enumerate(term_list())}
    total = {}

    def add(key, value):
        total[key] = value if key not in total else total[key] + value

    cosine, sine = None, None
    for m in range(COUNT):
        if m == 1:
            cosine, sine = unit_x, unit_y
        elif m > 1:
            cosine, sine = unit_x * cosine - unit_y * sine, unit_x * sine + unit_y * cosine
        sums = {}
        older, newer = None, None
        for l in range(m, COUNT):
            if l == m:
                now = None
            elif l == m + 1:
                now = unit_z
            elif l == m + 2:
                now = unit_z * newer - beta[l, m]
            else:
                now = unit_z * newer - beta[l, m] * older
            for kind in range(1 if m == 0 else 2):
                row = rows[kind, l, m]
                weight = coef[row : row + 1, :]
                weight = jnp.broadcast_to(weight, unit_z.shape)
                term = weight if now is None else weight * now
                key = (kind, (l - m) % 2)
                sums[key] = term if key not in sums else sums[key] + term
            older, newer = newer, now
        for (kind, odd), value in sums.items():
            if m > 0:
                value = value * (cosine, sine)[kind]
            add((m % 2 if keep_azimuth else 0, kind, odd), value)
    return total


def call(body, grid, in_specs, out_specs, out_shape, scratch, flops, name, **extra):
    return pl.pallas_call(
        body,
        grid=grid,
        in_specs=in_specs,
        out_specs=out_specs,
        out_shape=out_shape,
        scratch_shapes=scratch,
        name=name,
        cost_estimate=pl.CostEstimate(flops=flops, bytes_accessed=4 << 20, transcendentals=0),
        compiler_params=pltpu.CompilerParams(
            dimension_semantics=("arbitrary",) * len(grid), vmem_limit_bytes=56 << 20
        ),
    )


def whole(shape, memory=None):
    zeros = (0,) * len(shape)
    if memory is None:
        return pl.BlockSpec(shape, lambda *_: zeros)
    return pl.BlockSpec(shape, lambda *_: zeros, memory_space=memory)


def shards(charge_density):
    cells_a, cells_b, length = charge_density.shape
    groups_x, groups_y = lax.axis_size("gx"), lax.axis_size("gy")
    devices = groups_x * groups_y
    index_x, index_y = lax.axis_index("gx"), lax.axis_index("gy")
    tabs = constants(length)
    spacing = 1.0 / (length + 1)
    pack = max(1, 128 // cells_b)
    lanes = pack * cells_b
    wide = pack * length
    tiles = cells_a // pack
    depth = cells_b
    block = min(32, depth)
    blocks = depth // block
    modes = depth // groups_x
    ghosts = 2 * groups_x
    functions = COUNT + 2
    place = jnp.stack([index_x, index_y]).astype(jnp.int32)

    def const(name):
        return jnp.asarray(tabs[name].astype(np.float32))

    sine_high, sine_low = (jnp.asarray(t) for t in split_np(tabs["sine"]))
    sine_high = sine_high.reshape(groups_y, cells_b, length)
    sine_low = sine_low.reshape(groups_y, cells_b, length)
    diagonal = np.zeros((groups_y, pack, cells_b, pack, length))
    for item in range(pack):
        diagonal[:, item, :, item, :] = tabs["sine"].reshape(groups_y, cells_b, length)
    diagonal = diagonal.reshape(groups_y, lanes, wide)
    pair_high, pair_low = (jnp.asarray(t) for t in split_np(diagonal))
    back_high, back_low = (jnp.asarray(t) for t in split_np(diagonal.transpose(0, 2, 1)))

    many = min(2, tiles)

    def depth_body(place_ref, rho_ref, high_ref, low_ref, *rest):
        outs, table = rest[:groups_y], rest[groups_y]

        @pl.when(pl.program_id(0) == 0)
        def _():
            for shift in range(groups_y):
                peer = (place_ref[1] + shift) % groups_y
                table[0, pl.ds(shift * cells_b, cells_b), :] = high_ref[peer]
                table[1, pl.ds(shift * cells_b, cells_b), :] = low_ref[peer]

        value = rho_ref[...].reshape(many * lanes, length)
        high, low = split(value)
        result = mul(table[0], high, NT) + mul(table[1], high, NT) + mul(table[0], low, NT)
        for shift in range(groups_y):
            for item in range(many):
                outs[shift][item] = result[
                    shift * cells_b : (shift + 1) * cells_b, item * lanes : (item + 1) * lanes
                ]

    piece = jax.ShapeDtypeStruct((tiles, depth, lanes), F32)
    pieces = call(
        depth_body,
        (tiles // many,),
        [
            whole((2,), pltpu.SMEM),
            pl.BlockSpec((many * pack, cells_b, length), lambda t: (t, 0, 0)),
            whole((groups_y, cells_b, length)),
            whole((groups_y, cells_b, length)),
        ],
        [pl.BlockSpec((many, depth, lanes), lambda t: (t, 0, 0))] * groups_y,
        [piece] * groups_y,
        [pltpu.VMEM((2, length, length), BF16)],
        10**9,
        "depth_transform",
    )(place, charge_density, sine_high, sine_low)

    def exchange(parts):
        received = [parts[0]]
        for shift in range(1, groups_y):
            ring = [(source, (source + shift) % groups_y) for source in range(groups_y)]
            received.append(lax.ppermute(parts[shift], "gy", ring))
        return received

    received = exchange(pieces)

    eigen = const("eigen")
    eigen_depth = lax.dynamic_slice_in_dim(eigen, index_y * depth, depth)
    shift_value = eigen_depth[:, None] + eigen[None, :]
    sine64 = tabs["sine"]
    scale = 2.0 / (length + 1)
    hat_all = np.concatenate([tabs["legendre"] @ sine64, tabs["edges"]])
    padded = jnp.asarray(
        np.concatenate([np.zeros((1, length)), sine64, np.zeros((1, length))]).astype(np.float32)
    )
    left = lax.dynamic_slice_in_dim(padded, index_x * cells_a, 1)
    right = lax.dynamic_slice_in_dim(padded, (index_x + 1) * cells_a + 1, 1)
    hat_table = jnp.asarray((scale * hat_all).astype(np.float32))
    probe = jnp.concatenate([left * hat_table, right * hat_table])
    probe_rows = -(-2 * functions // 8) * 8
    probe = jnp.pad(probe, ((0, probe_rows - 2 * functions), (0, 0)))
    spots = []
    for slab in range(groups_x):
        spots += [slab * cells_a, (slab + 1) * cells_a + 1]
    lines = np.concatenate([np.zeros((1, length)), sine64, np.zeros((1, length))])[spots]
    green = (scale * lines[:, None, :] * lines[None, :, :]).reshape(ghosts * ghosts, length)
    green = jnp.asarray(green.astype(np.float32))
    kernel_column = jnp.broadcast_to(eigen[:, None], (length, length))

    def response(table, values, name):
        rows, count = table.shape[0], values.shape[0]
        group = min(8, count)

        def body(table_ref, column_ref, value_ref, out_ref):
            high, low = split(table_ref[...])
            for item in range(group):
                inverse = 1.0 / (column_ref[...] + value_ref[item : item + 1, :])
                inverse_high, inverse_low = split(inverse)
                answer = (
                    mul(high, inverse_high, NN)
                    + mul(low, inverse_high, NN)
                    + mul(high, inverse_low, NN)
                )
                out_ref[:, item, :] = answer

        return call(
            body,
            (count // group,),
            [
                whole((rows, length)),
                whole((length, length)),
                pl.BlockSpec((group, length), lambda k: (k, 0)),
            ],
            pl.BlockSpec((rows, group, length), lambda k: (0, k, 0)),
            jax.ShapeDtypeStruct((rows, count, length), F32),
            [],
            10**9,
            name,
        )(table, kernel_column, values)

    probe_table = response(probe, shift_value, "probe_table")
    own_values = lax.dynamic_slice_in_dim(shift_value, index_x * modes, modes)
    green_table = response(green, own_values, "green_table")

    def factor_body(value_ref, factor_ref, profile_ref):
        value = value_ref[...] + 2.0
        factor = 1.0 / value
        running = factor
        factor_ref[0] = factor
        profile_ref[0] = running
        for row in range(1, cells_a):
            factor = 1.0 / (value - factor)
            running = running * factor
            factor_ref[row] = factor
            profile_ref[row] = running
        for row in range(cells_a - 2, -1, -1):
            running = profile_ref[row] + factor_ref[row] * running
            profile_ref[row] = running

    field = jax.ShapeDtypeStruct((cells_a, depth, length), F32)
    factors, profile = call(
        factor_body,
        (1,),
        [whole((depth, length))],
        [whole((cells_a, depth, length))] * 2,
        [field, field],
        [],
        10**8,
        "factor_table",
    )(shift_value)

    legendre_local = lax.dynamic_slice_in_dim(const("legendre"), index_x * cells_a, cells_a, 1)
    ends = jnp.stack([index_x == 0, index_x == groups_x - 1]).astype(F32)
    fast, slow = const("fast"), const("slow")
    fast_local = lax.dynamic_slice_in_dim(fast, index_y * depth, depth)
    edges = const("edges")
    edges_local = lax.dynamic_slice_in_dim(edges, index_y * depth, depth, 1)
    edge_columns = jnp.broadcast_to(edges_local[:, :, None], (2, depth, length))
    edge_wide = jnp.broadcast_to(edges.T[:, :, None], (length, 2, 128)).reshape(length, 256)
    edge_rows = jnp.pad(edges, ((0, 6), (0, 0)))

    chunk = min(4, tiles)
    poly_rows = COUNT * block

    def solve_body(place_ref, leg_ref, end_ref, *refs):
        parts = refs[:groups_y]
        (
            high_ref,
            low_ref,
            factor_ref,
            probe_ref,
            slow_ref,
            fast_ref,
            fast_local_ref,
            column_ref,
            edge_ref,
            map_ref,
            mask_ref,
            field_ref,
            moment_ref,
            energy_ref,
            near_ref,
            weights,
            source,
            shaped,
            face_x,
            face_y,
            face_z,
        ) = refs[groups_y:]
        step = pl.program_id(0)

        @pl.when(step == 0)
        def _():
            for shift in range(groups_y):
                peer = (place_ref[1] + groups_y - shift) % groups_y
                weights[0, pl.ds(shift * lanes, lanes), :] = high_ref[peer]
                weights[1, pl.ds(shift * lanes, lanes), :] = low_ref[peer]
            face_x[...] = jnp.zeros_like(face_x)
            face_y[...] = jnp.zeros_like(face_y)
            face_z[...] = jnp.zeros_like(face_z)
            energy_ref[...] = jnp.zeros_like(energy_ref)

        for start in range(0, tiles, chunk):
            value = jnp.concatenate(
                [
                    part[start : start + chunk].reshape(chunk * block, lanes)
                    for part in parts
                ],
                axis=1,
            )
            high, low = split(value)
            result = (
                mul(high, weights[0], NN) + mul(high, weights[1], NN) + mul(low, weights[0], NN)
            ) * (spacing * spacing)
            for item in range(chunk):
                for inner in range(pack):
                    source[(start + item) * pack + inner] = result[
                        item * block : (item + 1) * block, inner * length : (inner + 1) * length
                    ]
        running = source[0] * factor_ref[0]
        field_ref[0] = running
        for row in range(1, cells_a):
            running = (source[row] + running) * factor_ref[row]
            field_ref[row] = running
        energy = source[cells_a - 1] * running
        for row in range(cells_a - 2, -1, -1):
            running = field_ref[row] + factor_ref[row] * running
            field_ref[row] = running
            energy = energy + source[row] * running
        energy = jnp.sum(energy.reshape(block // 8, 8, length), axis=0)
        for part in range(length // 128):
            energy_ref[...] += energy[:, part * 128 : (part + 1) * 128]
        near_ref[0] = field_ref[0]
        near_ref[1] = field_ref[cells_a - 1]
        for octet in range(block // 8):
            window = pl.ds(octet * 8, 8)
            first, last = field_ref[0, window, :], field_ref[cells_a - 1, window, :]
            sums = []
            for item in range(functions):
                value = probe_ref[item, window, :] * first
                sums.append(value + probe_ref[functions + item, window, :] * last)
            sums[COUNT] += end_ref[0] * first + end_ref[1] * last
            sums[COUNT + 1] += end_ref[1] * last - end_ref[0] * first
            for row in range(cells_a):
                value = field_ref[row, window, :]
                for item in range(COUNT):
                    sums[item] += leg_ref[item, row] * value
            for item in range(functions):
                shaped[item, window, :] = sums[item]

        rows = lax.broadcasted_iota(jnp.int32, (8, PAIRS), 0)
        for parity in range(2):
            value = exact(shaped[COUNT + parity], slow_ref[...], NN) * fast_local_ref[...]
            value = jnp.sum(value, axis=0, keepdims=True)
            face_x[...] += jnp.where(rows == parity, value, 0.0)
        stacked = shaped[0:COUNT].reshape(poly_rows, length)
        reduced = exact(stacked, edge_ref[...], NN)
        for parity in range(2):
            for item in range(COUNT):
                column = reduced[item * block : (item + 1) * block, parity * 128 : parity * 128 + 128]
                column = jnp.concatenate([column] * (PAIRS // 128), axis=1)
                value = jnp.sum(column * fast_local_ref[...], axis=0, keepdims=True)
                face_y[parity, item : item + 1, :] += value
                value = jnp.sum(column_ref[parity] * shaped[item], axis=0, keepdims=True)
                face_z[parity, item : item + 1, :] += value

        @pl.when(step == blocks - 1)
        def _():
            group = lax.broadcasted_iota(jnp.int32, (24, PAIRS), 0)
            order = lax.broadcasted_iota(jnp.int32, (24, PAIRS), 1)
            own = (order >= group * COUNT) & (order < (group + 1) * COUNT)
            moments = exact(face_x[...], map_ref[0], NN) * mask_ref[0]
            for face in (1, 2):
                stack = jnp.zeros((8, PAIRS), F32)
                for parity in range(2):
                    if face == 1:
                        value = face_y[parity]
                    else:
                        value = exact(face_z[parity], fast_ref[...], NN)
                    value = jnp.sum(jnp.where(own, value, 0.0), axis=0, keepdims=True)
                    stack = jnp.where(rows == parity, value, stack)
                moments = moments + exact(stack, map_ref[face], NN) * mask_ref[face]
            moments = jnp.sum(moments, axis=0, keepdims=True)
            moment_ref[...] = jnp.broadcast_to(moments, moment_ref.shape)

    by_depth = lambda k: (0, k, 0)
    field_spec = pl.BlockSpec((cells_a, block, length), by_depth)
    tile_spec = pl.BlockSpec((tiles, block, lanes), by_depth)
    solved, moments, energy_one, near_one = call(
        solve_body,
        (blocks,),
        [
            whole((2,), pltpu.SMEM),
            whole((COUNT, cells_a), pltpu.SMEM),
            whole((2,), pltpu.SMEM),
        ]
        + [tile_spec] * groups_y
        + [
            whole((groups_y, lanes, wide)),
            whole((groups_y, lanes, wide)),
            field_spec,
            pl.BlockSpec((probe_rows, block, length), by_depth),
            whole((length, PAIRS)),
            whole((length, PAIRS)),
            pl.BlockSpec((block, PAIRS), lambda k: (k, 0)),
            pl.BlockSpec((2, block, length), by_depth),
            whole((length, 256)),
            whole((3, PAIRS, TERMS)),
            whole((3, 8, TERMS)),
        ],
        [
            field_spec,
            whole((8, TERMS)),
            whole((8, 128)),
            pl.BlockSpec((2, block, length), by_depth),
        ],
        [
            field,
            jax.ShapeDtypeStruct((8, TERMS), F32),
            jax.ShapeDtypeStruct((8, 128), F32),
            jax.ShapeDtypeStruct((2, depth, length), F32),
        ],
        [
            pltpu.VMEM((2, groups_y * lanes, wide), BF16),
            pltpu.VMEM((cells_a, block, length), F32),
            pltpu.VMEM((functions, block, length), F32),
            pltpu.VMEM((8, PAIRS), F32),
            pltpu.VMEM((2, 24, PAIRS), F32),
            pltpu.VMEM((2, 24, length), F32),
        ],
        10**9,
        "solve_first",
    )(
        place,
        legendre_local,
        ends,
        *received,
        pair_high,
        pair_low,
        factors,
        probe_table,
        slow,
        fast,
        fast_local,
        edge_columns,
        edge_wide,
        const("maps"),
        const("masks"),
    )
    shared = lax.all_to_all(
        jnp.broadcast_to(moments[:1], (devices, TERMS)), ("gx", "gy"), 0, 0, tiled=True
    )

    scales = jnp.asarray(evaluation_scales()[0].astype(np.float32))
    cells = const("cells")
    half = length // 2
    cells_x = lax.dynamic_slice_in_dim(cells, index_x * cells_a, cells_a)
    upper = cells[half:]

    def unit(point_x, point_y, point_z, shape):
        points = [jnp.broadcast_to(p, shape) for p in (point_x, point_y, point_z)]
        inverse = 1.0 / jnp.sqrt(sum(p * p for p in points))
        return jnp.stack([p * inverse for p in points])

    unit_y = unit(cells_x[:, None], 0.5, upper[None, :], (cells_a, half))
    unit_z = unit(cells_x[:, None], upper[None, :], 0.5, (cells_a, half))
    unit_x = unit(0.5, upper[:, None], upper[None, :], (half, half))
    folded = const("folded")
    folded_local = lax.dynamic_slice_in_dim(folded.T, index_y * depth, depth)
    strip = 32

    def source_body(
        end_ref,
        share_ref,
        scale_ref,
        unit_y_ref,
        unit_z_ref,
        unit_x_ref,
        folded_ref,
        local_ref,
        row_ref,
        column_ref,
        factor_ref,
        solved_ref,
        total_ref,
        near_ref,
        energy_ref,
        coef,
        plane_x,
        plane_y,
        plane_z,
        lines_z,
        source,
    ):
        @pl.when(pl.program_id(0) == 0)
        def _():
            ones = jnp.ones((devices, 128), F32)
            coef[...] = exact(share_ref[...], ones, TN) * scale_ref[...]
            energy_ref[...] = jnp.zeros_like(energy_ref)
            for target, unit_ref, is_z in ((plane_y, unit_y_ref, False), (plane_z, unit_z_ref, True)):
                classes = evaluate(coef, unit_ref[0], unit_ref[1], unit_ref[2], False)
                for (_, kind, odd), value in classes.items():
                    row, column = (odd, kind) if is_z else (kind, odd)
                    target[
                        row * cells_a : (row + 1) * cells_a, column * half : (column + 1) * half
                    ] = value

            def one_strip(number, carry):
                window = pl.ds(number * strip, strip)
                classes = evaluate(
                    coef,
                    unit_x_ref[0, window, :],
                    unit_x_ref[1, window, :],
                    unit_x_ref[2, window, :],
                    True,
                )
                for (azimuth, kind, odd), value in classes.items():
                    plane_x[
                        (azimuth + kind) % 2,
                        pl.ds(kind * half + number * strip, strip),
                        odd * half : (odd + 1) * half,
                    ] = value
                return carry

            lax.fori_loop(0, half // strip, one_strip, 0)
            lines_z[...] = exact(plane_z[...], folded_ref[...], NN)

        lines_y = exact(local_ref[...], plane_y[...], NT)
        walls = []
        for parity in range(2):
            value = exact(local_ref[...], plane_x[parity], NT)
            walls.append(exact(value, folded_ref[...], NN))
        wall_first = end_ref[0] * (walls[0] - walls[1])
        wall_last = end_ref[1] * (walls[0] + walls[1])
        energy = jnp.zeros((block, length), F32)
        running = None
        for row in range(cells_a):
            value = jnp.zeros((block, length), F32)
            for parity in range(2):
                column = lines_y[:, parity * cells_a + row : parity * cells_a + row + 1]
                value = value + column * row_ref[parity : parity + 1, :]
                line = lines_z[parity * cells_a + row : parity * cells_a + row + 1, :]
                value = value + line * column_ref[parity]
            if row == 0:
                value = value + wall_first
            if row == cells_a - 1:
                value = value + wall_last
            energy = energy + value * solved_ref[row]
            running = value if running is None else value + running
            running = running * factor_ref[row]
            source[row] = running
        total_ref[cells_a - 1] = solved_ref[cells_a - 1] + running
        near_ref[1] = running
        for row in range(cells_a - 2, -1, -1):
            running = source[row] + factor_ref[row] * running
            total_ref[row] = solved_ref[row] + running
        near_ref[0] = running
        energy = jnp.sum(energy.reshape(block // 8, 8, length), axis=0)
        for part in range(length // 128):
            energy_ref[...] += energy[:, part * 128 : (part + 1) * 128]

    total, near_two, energy_two = call(
        source_body,
        (blocks,),
        [
            whole((2,), pltpu.SMEM),
            whole((devices, TERMS)),
            whole((TERMS, 128)),
            whole((3, cells_a, half)),
            whole((3, cells_a, half)),
            whole((3, half, half)),
            whole((length, length)),
            pl.BlockSpec((block, length), lambda k: (k, 0)),
            whole((8, length)),
            pl.BlockSpec((2, block, length), by_depth),
            field_spec,
            field_spec,
        ],
        [field_spec, pl.BlockSpec((2, block, length), by_depth), whole((8, 128))],
        [
            field,
            jax.ShapeDtypeStruct((2, depth, length), F32),
            jax.ShapeDtypeStruct((8, 128), F32),
        ],
        [
            pltpu.VMEM((TERMS, 128), F32),
            pltpu.VMEM((2, length, length), F32),
            pltpu.VMEM((2 * cells_a, length), F32),
            pltpu.VMEM((2 * cells_a, length), F32),
            pltpu.VMEM((2 * cells_a, length), F32),
            pltpu.VMEM((cells_a, block, length), F32),
        ],
        10**9,
        "face_sources",
    )(
        ends,
        shared,
        scales,
        unit_y,
        unit_z,
        unit_x,
        folded,
        folded_local,
        edge_rows,
        edge_columns,
        factors,
        solved,
    )

    nears = jnp.concatenate([near_one, near_two]).reshape(4, groups_x, modes, length)
    nears = jnp.transpose(nears, (1, 0, 2, 3))
    gathered = lax.all_to_all(nears, "gx", 0, 0, tiled=True)

    def ghost_body(near_ref, green_ref, one_ref, two_ref, out_ref):
        first = [near_ref[s, 0] for s in range(groups_x)]
        last = [near_ref[s, 1] for s in range(groups_x)]
        other_first = [near_ref[s, 2] for s in range(groups_x)]
        other_last = [near_ref[s, 3] for s in range(groups_x)]
        energy_one = jnp.zeros((modes, length), F32)
        energy_two = jnp.zeros((modes, length), F32)
        for slab in range(groups_x):
            for side in range(2):
                value = jnp.zeros((modes, length), F32)
                other = jnp.zeros((modes, length), F32)
                neighbour = slab + (1 if side else -1)
                if 0 <= neighbour < groups_x:
                    value = (first if side else last)[neighbour]
                    other = (other_first if side else other_last)[neighbour]
                    base = (2 * slab + side) * ghosts
                    for s in range(groups_x):
                        near, far = green_ref[base + 2 * s], green_ref[base + 2 * s + 1]
                        value = value + near * first[s] + far * last[s]
                        other = other + near * other_first[s] + far * other_last[s]
                energy_one = energy_one + value * (last if side else first)[slab]
                energy_two = energy_two + value * (other_last if side else other_first)[slab]
                out_ref[slab, side * modes : (side + 1) * modes, :] = value + other
        top = lax.broadcasted_iota(jnp.int32, (8, 128), 0) == 0
        for number, (local_ref, value) in enumerate(((one_ref, energy_one), (two_ref, energy_two))):
            value = jnp.sum(value, axis=0, keepdims=True)
            line = value[:, 0:128]
            for part in range(1, length // 128):
                line = line + value[:, part * 128 : (part + 1) * 128]
            tile = local_ref[...] + jnp.where(top, line, 0.0)
            for slab in range(groups_x):
                out_ref[slab, 2 * modes : 2 * modes + 8, number * 128 : (number + 1) * 128] = tile

    height = 2 * modes + 8
    answers = call(
        ghost_body,
        (1,),
        [
            whole((groups_x, 4, modes, length)),
            whole((ghosts * ghosts, modes, length)),
            whole((8, 128)),
            whole((8, 128)),
        ],
        whole((groups_x, height, length)),
        jax.ShapeDtypeStruct((groups_x, height, length), F32),
        [],
        10**8,
        "ghost_values",
    )(gathered, green_table, energy_one, energy_two)
    returned = lax.all_to_all(answers, "gx", 0, 0, tiled=True)
    ghost = jnp.stack(
        [
            returned[:, :modes].reshape(depth, length),
            returned[:, modes : 2 * modes].reshape(depth, length),
        ]
    )
    energy_tile = jnp.sum(returned[:, 2 * modes :, :256], axis=0)

    def back_body(place_ref, total_ref, profile_ref, ghost_ref, high_ref, low_ref, *rest):
        outs, weights = rest[:groups_y], rest[groups_y]

        @pl.when(pl.program_id(0) == 0)
        def _():
            for shift in range(groups_y):
                peer = (place_ref[1] + shift) % groups_y
                weights[0, :, shift * lanes : (shift + 1) * lanes] = high_ref[peer]
                weights[1, :, shift * lanes : (shift + 1) * lanes] = low_ref[peer]

        for start in range(0, tiles, chunk):
            parts = []
            for item in range(start, start + chunk):
                inner = []
                for row in range(item * pack, (item + 1) * pack):
                    inner.append(
                        total_ref[row]
                        + profile_ref[row] * ghost_ref[0]
                        + profile_ref[cells_a - 1 - row] * ghost_ref[1]
                    )
                parts.append(jnp.concatenate(inner, axis=1))
            high, low = split(jnp.concatenate(parts, axis=0))
            result = (
                mul(high, weights[0], NN) + mul(high, weights[1], NN) + mul(low, weights[0], NN)
            )
            for shift in range(groups_y):
                for item in range(chunk):
                    outs[shift][start + item] = result[
                        item * block : (item + 1) * block, shift * lanes : (shift + 1) * lanes
                    ]

    parts = call(
        back_body,
        (blocks,),
        [
            whole((2,), pltpu.SMEM),
            field_spec,
            field_spec,
            pl.BlockSpec((2, block, length), by_depth),
            whole((groups_y, wide, lanes)),
            whole((groups_y, wide, lanes)),
        ],
        [tile_spec] * groups_y,
        [piece] * groups_y,
        [pltpu.VMEM((2, wide, groups_y * lanes), BF16)],
        10**9,
        "second_back",
    )(place, total, profile, ghost, back_high, back_low)
    returned = exchange(parts)
    tiles_all = sum(exchange([energy_tile] * groups_y))

    norm = (2.0 / (length + 1)) ** 2

    def last_body(place_ref, *refs):
        blocks_in = refs[:groups_y]
        high_ref, low_ref, out_ref, table = refs[groups_y:]

        @pl.when(pl.program_id(0) == 0)
        def _():
            for shift in range(groups_y):
                peer = (place_ref[1] + groups_y - shift) % groups_y
                table[0, pl.ds(shift * cells_b, cells_b), :] = high_ref[peer]
                table[1, pl.ds(shift * cells_b, cells_b), :] = low_ref[peer]

        for item in range(many):
            value = jnp.concatenate([part[item] for part in blocks_in], axis=0)
            high, low = split(value.T)
            result = mul(high, table[0], NN) + mul(high, table[1], NN) + mul(low, table[0], NN)
            out_ref[item * pack : (item + 1) * pack] = (result * norm).reshape(
                pack, cells_b, length
            )

    potential = call(
        last_body,
        (tiles // many,),
        [whole((2,), pltpu.SMEM)]
        + [pl.BlockSpec((many, depth, lanes), lambda t: (t, 0, 0))] * groups_y
        + [whole((groups_y, cells_b, length))] * 2,
        pl.BlockSpec((many * pack, cells_b, length), lambda t: (t, 0, 0)),
        jax.ShapeDtypeStruct(charge_density.shape, F32),
        [pltpu.VMEM((2, length, length), BF16)],
        10**9,
        "depth_back",
    )(place, *returned, sine_high, sine_low)
    sums = jnp.stack([jnp.sum(tiles_all[:, :128]), jnp.sum(tiles_all[:, 128:])])
    sums = sums * (spacing * (2.0 / (length + 1)) ** 2)
    return potential, jnp.stack([sums[0], sums[0] + sums[1]])


def solution(mesh):
    placed = (P("gx", "gy", None),)
    return jax.shard_map(
        shards, mesh=mesh, in_specs=placed, out_specs=(P("gx", "gy", None), P()), check_vma=False
    )
```

```python
import functools
import math

import jax
import jax.numpy as jnp
import numpy as np
from jax import lax
from jax.experimental import pallas as pl
from jax.experimental.pallas import tpu as pltpu
from jax.sharding import PartitionSpec as P

ORDER = 16
COUNT = ORDER + 1
PAIRS = 256
TERMS = 384
outer_ratio = 1.1
radius_scale = math.sqrt(3.0) / 2.0
F32 = jnp.float32
BF16 = jnp.bfloat16
EXACT = lax.Precision.HIGHEST


NN = (((1,), (0,)), ((), ()))
NT = (((1,), (1,)), ((), ()))
TN = (((0,), (0,)), ((), ()))


def pair_list():
    return [(p, q) for p in range(COUNT) for q in range(COUNT - p)]


def term_list():
    terms = [(0, l, m) for m in range(COUNT) for l in range(m, COUNT)]
    terms += [(1, l, m) for m in range(1, COUNT) for l in range(m, COUNT)]
    return terms


def split_np(table):
    import ml_dtypes

    high = table.astype(np.float32).astype(ml_dtypes.bfloat16)
    low = (table - high.astype(np.float64)).astype(np.float32).astype(ml_dtypes.bfloat16)
    return high, low


def split(value):
    high = value.astype(BF16)
    return high, (value - high.astype(F32)).astype(BF16)


def mul(left, right, dims):
    return lax.dot_general(left, right, dims, preferred_element_type=F32)


def triple(left, high, low, dims):
    first, second = split(left)
    return mul(first, high, dims) + mul(first, low, dims) + mul(second, high, dims)


def exact(left, right, dims):
    return lax.dot_general(left, right, dims, precision=EXACT, preferred_element_type=F32)


def solid_values(x, y, z):
    squared = x * x + y * y + z * z
    cosine, sine = {}, {}
    cosine[0, 0], sine[0, 0] = np.ones_like(x), np.zeros_like(x)
    for l in range(1, COUNT):
        scale = math.sqrt((2 * l - 1) / (2.0 * l)) if l > 1 else 1.0
        cosine[l, l] = scale * (x * cosine[l - 1, l - 1] - y * sine[l - 1, l - 1])
        sine[l, l] = scale * (x * sine[l - 1, l - 1] + y * cosine[l - 1, l - 1])
    for table in (cosine, sine):
        for m in range(COUNT):
            for l in range(m + 1, COUNT):
                older = table[l - 2, m] if l - 2 >= m else np.zeros_like(x)
                table[l, m] = (
                    (2 * l - 1) * z * table[l - 1, m]
                    - math.sqrt((l - 1) ** 2 - m * m) * squared * older
                ) / math.sqrt(l * l - m * m)
    return [(cosine, sine)[kind][l, m] for kind, l, m in term_list()]


@functools.cache
def constants(length):
    step = length + 1
    index = np.arange(length) + 1
    sine = np.sin(np.pi * ((index[:, None] * index[None, :]) % (2 * step)) / step)
    eigen = 4.0 * np.sin(np.pi * index / (2.0 * step)) ** 2
    cells = (np.arange(length) - (length - 1) / 2.0) / step
    legendre = np.stack(
        [np.polynomial.legendre.legval(2 * cells, np.eye(COUNT)[p]) for p in range(COUNT)]
    )
    hat = legendre @ sine
    edges = np.stack([sine[0] + sine[-1], sine[-1] - sine[0]])
    lookup = np.concatenate([hat, edges])
    columns = np.zeros((length, 128))
    columns[:, : COUNT + 2] = lookup.T
    spread = np.zeros((2, 128, PAIRS))
    own = np.zeros((2, 24, PAIRS))
    for spot, pair in enumerate(pair_list()):
        for kind in range(2):
            spread[kind, pair[kind], spot] = 1.0
            own[kind, pair[kind], spot] = 1.0
    nodes, weights = np.polynomial.legendre.leggauss(COUNT + 3)
    basis = np.stack([np.polynomial.legendre.legval(nodes, np.eye(COUNT)[p]) for p in range(COUNT)])
    project = basis * weights[None, :] * (2 * np.arange(COUNT)[:, None] + 1) / 2.0
    first, second = np.meshgrid(nodes / 2.0, nodes / 2.0, indexing="ij")
    half = np.full_like(first, 0.5)
    terms = term_list()
    scale = (1.0 / step) * (2.0 / step) ** 2
    maps = np.zeros((3, PAIRS, TERMS))
    places = [(half, first, second), (first, half, second), (first, second, half)]
    for face, place in enumerate(places):
        for column, values in enumerate(solid_values(*place)):
            degree = terms[column][1]
            expansion = project @ values @ project.T
            for spot, pair in enumerate(pair_list()):
                maps[face, spot, column] = scale * expansion[pair] / radius_scale**degree
    masks = np.zeros((3, 8, TERMS))
    for column, (kind, l, m) in enumerate(terms):
        masks[0, (m + kind) % 2, column] = 1.0
        masks[1, kind, column] = 1.0
        masks[2, (l - m) % 2, column] = 1.0
    folded = np.zeros((2, length // 2, length))
    parity = np.arange(length) % 2
    upper = 2.0 * sine[length // 2 :]
    folded[0] = upper * (parity == 0)
    folded[1] = upper * (parity == 1)
    return dict(
        sine=sine,
        eigen=eigen,
        cells=cells,
        legendre=legendre,
        columns=columns,
        spread=spread,
        own=own,
        edges=edges,
        maps=maps,
        masks=masks,
        folded=folded.reshape(length, length),
    )


def evaluation_scales():
    sector, running = [1.0], 1.0
    for l in range(1, COUNT):
        running *= math.sqrt((2 * l - 1) / (2.0 * l)) if l > 1 else 1.0
        sector.append(running)
    kappa, beta = {}, {}
    for m in range(COUNT):
        kappa[m, m] = sector[m]
        previous = 1.0
        for l in range(m + 1, COUNT):
            near = (2 * l - 1) / math.sqrt(l * l - m * m)
            far = math.sqrt((l - 1) ** 2 - m * m) / math.sqrt(l * l - m * m)
            kappa[l, m] = kappa[l - 1, m] * near
            beta[l, m] = far / (near * previous) if l >= m + 2 else 0.0
            previous = near
    scales = np.zeros((8, TERMS))
    for row, (_, l, m) in enumerate(term_list()):
        factor = 1.0 if m == 0 else 2.0
        weight = factor / (4.0 * math.pi * radius_scale * outer_ratio ** (l + 1))
        scales[:, row] = weight * kappa[l, m]
    return scales, beta


def evaluate(coef, unit_x, unit_y, unit_z, keep_azimuth):
    beta = evaluation_scales()[1]
    rows = {term: row for row, term in enumerate(term_list())}
    total = {}

    def add(key, value):
        total[key] = value if key not in total else total[key] + value

    cosine, sine = None, None
    for m in range(COUNT):
        if m == 1:
            cosine, sine = unit_x, unit_y
        elif m > 1:
            cosine, sine = unit_x * cosine - unit_y * sine, unit_x * sine + unit_y * cosine
        sums = {}
        older, newer = None, None
        for l in range(m, COUNT):
            if l == m:
                now = None
            elif l == m + 1:
                now = unit_z
            elif l == m + 2:
                now = unit_z * newer - beta[l, m]
            else:
                now = unit_z * newer - beta[l, m] * older
            for kind in range(1 if m == 0 else 2):
                row = rows[kind, l, m]
                weight = coef[row : row + 1, :]
                weight = jnp.broadcast_to(weight, unit_z.shape)
                term = weight if now is None else weight * now
                key = (kind, (l - m) % 2)
                sums[key] = term if key not in sums else sums[key] + term
            older, newer = newer, now
        for (kind, odd), value in sums.items():
            if m > 0:
                value = value * (cosine, sine)[kind]
            add((m % 2 if keep_azimuth else 0, kind, odd), value)
    return total


RESIDENT = pl.BlockSpec(memory_space=pltpu.VMEM)
SCALARS = pl.BlockSpec(memory_space=pltpu.SMEM)


def call(body, grid, in_specs, out_specs, out_shape, scratch, flops, name, aliases=None, limit=24):
    kernel = pl.pallas_call(
        body,
        grid=grid,
        in_specs=in_specs,
        out_specs=out_specs,
        out_shape=out_shape,
        scratch_shapes=scratch,
        name=name,
        input_output_aliases=aliases or {},
        cost_estimate=pl.CostEstimate(flops=flops, bytes_accessed=4 << 20, transcendentals=0),
        compiler_params=pltpu.CompilerParams(
            dimension_semantics=("arbitrary",) * len(grid), vmem_limit_bytes=limit << 20
        ),
    )

    def run(*args):
        placed = []
        for arg, spec in zip(args, in_specs):
            if spec is RESIDENT:
                arg = pltpu.with_memory_space_constraint(arg, pltpu.VMEM)
            elif spec.block_shape is not None:
                arg = pltpu.with_memory_space_constraint(arg, pltpu.HBM)
            placed.append(arg)
        return kernel(*placed)

    return run


def kept(*shape):
    return pltpu.VMEM(shape, F32)


def shards(charge_density):
    cells_a, cells_b, length = charge_density.shape
    groups_x, groups_y = lax.axis_size("gx"), lax.axis_size("gy")
    devices = groups_x * groups_y
    index_x, index_y = lax.axis_index("gx"), lax.axis_index("gy")
    tabs = constants(length)
    spacing = 1.0 / (length + 1)
    pack = max(1, 128 // cells_b)
    lanes = pack * cells_b
    wide = pack * length
    tiles = cells_a // pack
    depth = cells_b
    block = min(32, depth)
    blocks = depth // block
    modes = depth // groups_x
    ghosts = 2 * groups_x
    functions = COUNT + 2
    place = jnp.stack([index_x, index_y]).astype(jnp.int32)

    def const(name):
        return jnp.asarray(tabs[name].astype(np.float32))

    sine_high, sine_low = (jnp.asarray(t) for t in split_np(tabs["sine"]))
    sine_high = sine_high.reshape(groups_y, cells_b, length)
    sine_low = sine_low.reshape(groups_y, cells_b, length)
    halves = 2 if tiles % 4 == 0 else 1
    part_tiles = tiles // halves

    pair_limit = 24 if wide <= 512 else 44

    def fill_pairs(weights, high_ref, low_ref, index_y):
        weights[...] = jnp.zeros_like(weights)
        for shift in range(groups_y):
            peer = index_y ^ shift
            for item in range(pack):
                rows = pl.ds(shift * lanes + item * cells_b, cells_b)
                weights[0, rows, item * length : (item + 1) * length] = high_ref[peer]
                weights[1, rows, item * length : (item + 1) * length] = low_ref[peer]

    many = min(4, part_tiles)

    def depth_body(place_ref, rho_ref, high_ref, low_ref, *rest):
        outs, table = rest[:groups_y], rest[groups_y]

        @pl.when(pl.program_id(0) == 0)
        def _():
            for shift in range(groups_y):
                peer = place_ref[1] ^ shift
                table[0, pl.ds(shift * cells_b, cells_b), :] = high_ref[peer]
                table[1, pl.ds(shift * cells_b, cells_b), :] = low_ref[peer]

        value = rho_ref[...].reshape(many * lanes, length)
        high, low = split(value)
        result = mul(table[0], high, NT) + mul(table[1], high, NT) + mul(table[0], low, NT)
        start = pl.program_id(0) * many
        for shift in range(groups_y):
            for item in range(many):
                outs[shift][start + item] = result[
                    shift * cells_b : (shift + 1) * cells_b, item * lanes : (item + 1) * lanes
                ]

    piece = kept(part_tiles, depth, lanes)
    table_spec = pl.BlockSpec((groups_y, cells_b, length), lambda t: (0, 0, 0))

    def depth_transform(number):
        steps = part_tiles // many
        return call(
            depth_body,
            (steps,),
            [
                SCALARS,
                pl.BlockSpec((many * pack, cells_b, length), lambda t: (t + number * steps, 0, 0)),
                table_spec,
                table_spec,
            ],
            [RESIDENT] * groups_y,
            [piece] * groups_y,
            [pltpu.VMEM((2, length, length), BF16)],
            10**9,
            "depth_transform",
        )(
            place,
            charge_density,
            sine_high,
            sine_low,
        )

    def exchange(parts):
        received = [parts[0]]
        for shift in range(1, groups_y):
            ring = [(source, source ^ shift) for source in range(groups_y)]
            received.append(lax.ppermute(parts[shift], "gy", ring))
        return received

    received = [exchange(depth_transform(number)) for number in range(halves)]

    half = length // 2
    sine64 = tabs["sine"]
    scale = 2.0 / (length + 1)
    hat_all = scale * np.concatenate([tabs["legendre"] @ sine64, tabs["edges"]])
    hat_pad = -(-functions // 8) * 8
    hat_all = np.concatenate([hat_all, np.zeros((hat_pad - functions, length))])
    blank = np.zeros((1, length))
    lines = np.concatenate([blank, sine64, blank])
    spots = []
    for slab in range(groups_x):
        spots += [slab * cells_a, (slab + 1) * cells_a + 1]
    green_lines = lines[spots]
    green = (scale * green_lines[:, None, :] * green_lines[None, :, :]).reshape(-1, length)
    eigen_column = np.broadcast_to(tabs["eigen"][:, None], (length, length))
    eigen_row = np.broadcast_to(tabs["eigen"][None, :], (8, length))
    cell_column = np.broadcast_to(tabs["cells"][:, None], (length, half))
    cell_row = np.broadcast_to(tabs["cells"][None, half:], (8, half))

    def put(table):
        return jnp.asarray(np.ascontiguousarray(table).astype(np.float32))

    def prepare_body(
        place_ref,
        column_ref,
        row_ref,
        line_ref,
        hat_ref,
        green_high_ref,
        green_low_ref,
        cell_column_ref,
        cell_row_ref,
        sine_high_ref,
        sine_low_ref,
        factor_ref,
        profile_ref,
        probe_ref,
        green_ref,
        unit_y_ref,
        unit_z_ref,
        unit_x_ref,
        pair_ref,
        table_ref,
        values,
        probe_high,
        probe_low,
    ):
        index_x, index_y = place_ref[0], place_ref[1]
        fill_pairs(pair_ref, sine_high_ref, sine_low_ref, index_y)
        for shift in range(groups_y):
            peer = index_y ^ shift
            table_ref[0, pl.ds(shift * cells_b, cells_b), :] = sine_high_ref[peer]
            table_ref[1, pl.ds(shift * cells_b, cells_b), :] = sine_low_ref[peer]
        own = pl.ds(pl.multiple_of(index_y * depth, depth), depth)
        values[...] = column_ref[own, :] + row_ref[0:1, :]
        value = values[...] + 2.0
        factor = 1.0 / value
        running = factor
        factor_ref[0] = factor
        profile_ref[0] = running
        for row in range(1, cells_a):
            factor = 1.0 / (value - factor)
            running = running * factor
            factor_ref[row] = factor
            profile_ref[row] = running
        for row in range(cells_a - 2, -1, -1):
            running = profile_ref[row] + factor_ref[row] * running
            profile_ref[row] = running
        for side in range(2):
            spot = index_x * cells_a + side * (cells_a + 1)
            table = line_ref[pl.ds(spot, 1), :] * hat_ref[...]
            high, low = split(table)
            probe_high[side * hat_pad : (side + 1) * hat_pad] = high
            probe_low[side * hat_pad : (side + 1) * hat_pad] = low

        def inverse_of(spot):
            return split(1.0 / (column_ref[...] + values[pl.ds(spot, 1), :]))

        def probe_step(number, carry):
            high, low = inverse_of(number)
            answer = (
                mul(probe_high[...], high, NN)
                + mul(probe_low[...], high, NN)
                + mul(probe_high[...], low, NN)
            )
            probe_ref[pl.ds(number, 1)] = answer[None]
            return carry

        lax.fori_loop(0, depth, probe_step, 0)

        def green_step(number, carry):
            high, low = inverse_of(index_x * modes + number)
            answer = (
                mul(green_high_ref[...], high, NN)
                + mul(green_low_ref[...], high, NN)
                + mul(green_high_ref[...], low, NN)
            )
            green_ref[pl.ds(number, 1)] = answer[None]
            return carry

        lax.fori_loop(0, modes, green_step, 0)
        here = pl.ds(pl.multiple_of(index_x * cells_a, cells_a), cells_a)
        middle = jnp.full((8, half), 0.5, F32)[0:1]
        along = cell_row_ref[0:1, :]
        for target, first, second, third in (
            (unit_y_ref, cell_column_ref[here, :], middle, along),
            (unit_z_ref, cell_column_ref[here, :], along, middle),
            (unit_x_ref, middle, cell_column_ref[half:, :], along),
        ):
            inverse = 1.0 / jnp.sqrt(first * first + second * second + third * third)
            target[0] = first * inverse
            target[1] = second * inverse
            target[2] = third * inverse

    field = kept(cells_a, depth, length)
    green_high, green_low = (jnp.asarray(t) for t in split_np(green))
    inputs = (
        put(eigen_column),
        put(eigen_row),
        put(lines),
        put(hat_all),
        green_high,
        green_low,
        put(cell_column),
        put(cell_row),
        sine_high,
        sine_low,
    )

    def block_of(array):
        zeros = (0,) * array.ndim
        return pl.BlockSpec(array.shape, lambda k: zeros)

    tables = call(
        prepare_body,
        (1,),
        [SCALARS] + [block_of(array) for array in inputs],
        [RESIDENT] * 9,
        [
            field,
            field,
            kept(depth, 2 * hat_pad, length),
            kept(modes, ghosts * ghosts, length),
            kept(3, cells_a, half),
            kept(3, cells_a, half),
            kept(3, half, half),
            pltpu.VMEM((2, groups_y * lanes, wide), BF16),
            pltpu.VMEM((2, length, length), BF16),
        ],
        [
            pltpu.VMEM((depth, length), F32),
            pltpu.VMEM((2 * hat_pad, length), BF16),
            pltpu.VMEM((2 * hat_pad, length), BF16),
        ],
        10**10,
        "prepare_tables",
        limit=pair_limit,
    )(place, *inputs)
    legendre = put(tabs["legendre"])
    edge_rows = put(np.concatenate([tabs["edges"], np.zeros((6, length))]))
    edge_columns = put(np.broadcast_to(tabs["edges"][:, :, None], (2, length, 128)))
    column_high, column_low = (jnp.asarray(t) for t in split_np(tabs["columns"]))
    lookup = np.zeros((groups_y, 24, depth))
    lookup[:, : COUNT + 2] = (
        tabs["columns"][:, : COUNT + 2].T.reshape(COUNT + 2, groups_y, depth).transpose(1, 0, 2)
    )
    lookup = lookup.reshape(groups_y, 24, blocks, block).transpose(0, 2, 1, 3)
    lookup_high, lookup_low = (jnp.asarray(t) for t in split_np(lookup))
    spread = jnp.asarray(tabs["spread"].astype(np.float32)).astype(BF16)
    map_high, map_low = (jnp.asarray(t) for t in split_np(tabs["maps"]))
    received[-1], tables = lax.optimization_barrier((received[-1], tables))
    factors, profile, probe_table, green_table, unit_y, unit_z, unit_x, pairs, table = tables

    def second_body(*refs):
        blocks_in = refs[:groups_y]
        weights, out_ref = refs[groups_y:]
        for start in range(0, depth, block):
            value = jnp.concatenate(
                [
                    part[:, start : start + block, :].reshape(part_tiles * block, lanes)
                    for part in blocks_in
                ],
                axis=1,
            )
            result = triple(value, weights[0], weights[1], NN) * (spacing * spacing)
            for item in range(part_tiles):
                for inner in range(pack):
                    out_ref[item * pack + inner, start : start + block, :] = result[
                        item * block : (item + 1) * block, inner * length : (inner + 1) * length
                    ]

    part_cells = part_tiles * pack
    sources = [
        call(
            second_body,
            (1,),
            [RESIDENT] * (groups_y + 1),
            RESIDENT,
            kept(part_cells, depth, length),
            [],
            10**9,
            "second_transform",
            limit=pair_limit,
        )(*parts, pairs)
        for parts in received
    ]


    def solve_body(place_ref, leg_ref, *refs):
        given = refs[:halves]
        (
            factor_ref,
            probe_ref,
            column_high_ref,
            column_low_ref,
            lookup_high_ref,
            lookup_low_ref,
            spread_ref,
            own_ref,
            map_high_ref,
            map_low_ref,
            mask_ref,
            field_ref,
            moment_ref,
            energy_ref,
            tensor,
        ) = refs[halves:]
        index_x, index_y = place_ref[0], place_ref[1]
        begin = jnp.where(index_x == 0, 1.0, 0.0)
        finish = jnp.where(index_x == groups_x - 1, 1.0, 0.0)
        step = pl.program_id(0)
        base = pl.multiple_of(step * block, block)
        window = pl.ds(base, block)

        @pl.when(step == 0)
        def _():
            tensor[...] = jnp.zeros_like(tensor)
            energy_ref[...] = jnp.zeros_like(energy_ref)

        def source(row):
            return given[row // part_cells][row % part_cells, window, :]

        running = source(0) * factor_ref[0, window, :]
        field_ref[0, window, :] = running
        for row in range(1, cells_a):
            running = (source(row) + running) * factor_ref[row, window, :]
            field_ref[row, window, :] = running
        energy = source(cells_a - 1) * running
        for row in range(cells_a - 2, -1, -1):
            running = field_ref[row, window, :] + factor_ref[row, window, :] * running
            field_ref[row, window, :] = running
            energy = energy + source(row) * running
        energy = jnp.sum(energy.reshape(block // 8, 8, length), axis=0)
        for part in range(length // 128):
            energy_ref[...] += energy[:, part * 128 : (part + 1) * 128]
        first, last = field_ref[0, window, :], field_ref[cells_a - 1, window, :]
        table_high, table_low = column_high_ref[...], column_low_ref[...]
        rows_high = lookup_high_ref[index_y, step]
        rows_low = lookup_low_ref[index_y, step]

        def contract(stack, count):
            answer = triple(stack, table_high, table_low, NN)
            upper, lower = split(answer)
            outs = []
            for item in range(count):
                high = upper[item * block : (item + 1) * block]
                low = lower[item * block : (item + 1) * block]
                outs.append(
                    mul(rows_high, high, NN) + mul(rows_low, high, NN) + mul(rows_high, low, NN)
                )
            return outs

        many_rows = min(16, cells_a)
        for start in range(0, cells_a, many_rows):
            stack = field_ref[start : start + many_rows, window, :].reshape(
                many_rows * block, length
            )
            outs = contract(stack, many_rows)
            for item in range(COUNT):
                value = tensor[item]
                for inner, out in enumerate(outs):
                    value = value + leg_ref[item, index_x * cells_a + start + inner] * out
                tensor[item] = value
            if start == 0:
                tensor[COUNT] += begin * outs[0]
                tensor[COUNT + 1] -= begin * outs[0]
            if start + many_rows == cells_a:
                tensor[COUNT] += finish * outs[-1]
                tensor[COUNT + 1] += finish * outs[-1]
        group = 10
        for start in range(0, functions, group):
            items = range(start, min(start + group, functions))
            stack = jnp.concatenate(
                [
                    probe_ref[window, item, :] * first + probe_ref[window, hat_pad + item, :] * last
                    for item in items
                ],
                axis=0,
            )
            for item, out in zip(items, contract(stack, len(items))):
                tensor[item] += out

        @pl.when(step == blocks - 1)
        def _():
            rows = lax.broadcasted_iota(jnp.int32, (8, PAIRS), 0)

            def flatten(matrix, kind):
                high, low = split(matrix)
                answer = mul(high, spread_ref[kind], NN) + mul(low, spread_ref[kind], NN)
                return jnp.sum(answer * own_ref[1 - kind], axis=0, keepdims=True)

            moments = jnp.zeros((8, TERMS), F32)
            for face in range(3):
                stack = jnp.zeros((8, PAIRS), F32)
                for parity in range(2):
                    if face == 0:
                        value = flatten(tensor[COUNT + parity], 0)
                    elif face == 1:
                        value = jnp.zeros((1, PAIRS), F32)
                        for item in range(COUNT):
                            column = tensor[item, :, COUNT + parity : COUNT + parity + 1]
                            chosen = own_ref[0, item : item + 1, :] * own_ref[1]
                            value = value + jnp.sum(column * chosen, axis=0, keepdims=True)
                    else:
                        matrix = jnp.concatenate(
                            [
                                tensor[item, COUNT + parity : COUNT + parity + 1, :]
                                for item in range(COUNT)
                            ]
                            + [jnp.zeros((24 - COUNT, 128), F32)],
                            axis=0,
                        )
                        high, low = split(matrix)
                        answer = mul(high, spread_ref[1], NN) + mul(low, spread_ref[1], NN)
                        value = jnp.sum(answer * own_ref[0], axis=0, keepdims=True)
                    stack = jnp.where(rows == parity, value, stack)
                moments = moments + triple(stack, map_high_ref[face], map_low_ref[face], NN) * (
                    mask_ref[face]
                )
            moments = jnp.sum(moments, axis=0, keepdims=True)
            moment_ref[...] = jnp.broadcast_to(moments[None], moment_ref.shape)

    solved, moments, energy_one = call(
        solve_body,
        (blocks,),
        [SCALARS] * 2 + [RESIDENT] * (halves + 11),
        [RESIDENT] * 3,
        [field, kept(devices, 1, TERMS), kept(8, 128)],
        [
            pltpu.VMEM((24, 24, 128), F32),
        ],
        10**9,
        "solve_first",
    )(
        place,
        legendre,
        *sources,
        factors,
        probe_table,
        column_high,
        column_low,
        lookup_high,
        lookup_low,
        spread,
        const("own"),
        map_high,
        map_low,
        const("masks"),
    )
    shared = lax.all_to_all(moments, ("gx", "gy"), 0, 0, tiled=True)

    scales = jnp.asarray(evaluation_scales()[0].astype(np.float32))
    folded_high, folded_low = (jnp.asarray(t) for t in split_np(tabs["folded"]))
    local_high, local_low = (
        jnp.asarray(np.ascontiguousarray(t.T).reshape(groups_y, depth, length))
        for t in split_np(tabs["folded"])
    )
    strip = 32
    shares_count = block // modes

    def source_body(
        place_ref,
        share_ref,
        scale_ref,
        unit_y_ref,
        unit_z_ref,
        unit_x_ref,
        folded_high_ref,
        folded_low_ref,
        local_high_ref,
        local_low_ref,
        row_ref,
        column_ref,
        factor_ref,
        solved_ref,
        total_ref,
        near_ref,
        energy_ref,
        coef,
        plane_x,
        plane_y,
        plane_z,
        lines_y,
        lines_z,
        walls,
        source,
    ):
        index_x, index_y = place_ref[0], place_ref[1]
        begin = jnp.where(index_x == 0, 1.0, 0.0)
        finish = jnp.where(index_x == groups_x - 1, 1.0, 0.0)

        step = pl.program_id(0)
        window = pl.ds(pl.multiple_of(step * block, block), block)

        @pl.when(step == 0)
        def _():
            ones = jnp.full((8, 128), 0.125, F32)
            shares = jnp.sum(share_ref[...], axis=0) * scale_ref[...]
            coef[...] = exact(shares, ones, TN)
            energy_ref[...] = jnp.zeros_like(energy_ref)
            for target, unit_ref, is_z in ((plane_y, unit_y_ref, False), (plane_z, unit_z_ref, True)):
                classes = evaluate(coef, unit_ref[0], unit_ref[1], unit_ref[2], False)
                for (_, kind, odd), value in classes.items():
                    row, column = (odd, kind) if is_z else (kind, odd)
                    target[
                        row * cells_a : (row + 1) * cells_a, column * half : (column + 1) * half
                    ] = value

            def one_strip(number, carry):
                window = pl.ds(number * strip, strip)
                classes = evaluate(
                    coef,
                    unit_x_ref[0, window, :],
                    unit_x_ref[1, window, :],
                    unit_x_ref[2, window, :],
                    True,
                )
                for (azimuth, kind, odd), value in classes.items():
                    plane_x[
                        (azimuth + kind) % 2,
                        pl.ds(kind * half + number * strip, strip),
                        odd * half : (odd + 1) * half,
                    ] = value
                return carry

            lax.fori_loop(0, half // strip, one_strip, 0)
            folded_tables = folded_high_ref[...], folded_low_ref[...]
            local_tables = local_high_ref[index_y], local_low_ref[index_y]

            def across(plane):
                upper, lower = split(plane)
                high, low = local_tables
                return mul(high, upper, NT) + mul(low, upper, NT) + mul(high, lower, NT)

            lines_z[...] = triple(plane_z[...], *folded_tables, NN)
            lines_y[...] = across(plane_y[...])
            even, odd = (triple(across(plane_x[parity]), *folded_tables, NN) for parity in range(2))
            walls[0] = begin * (even - odd)
            walls[1] = finish * (even + odd)

        here = pl.ds(pl.multiple_of(index_y * depth + step * block, block), block)
        columns = [
            jnp.concatenate([column_ref[parity, here, :]] * (length // 128), axis=1)
            for parity in range(2)
        ]
        line_block = lines_y[window, :]
        energy = jnp.zeros((block, length), F32)
        running = None
        for row in range(cells_a):
            value = jnp.zeros((block, length), F32)
            for parity in range(2):
                column = line_block[:, parity * cells_a + row : parity * cells_a + row + 1]
                value = value + column * row_ref[parity : parity + 1, :]
                line = lines_z[parity * cells_a + row : parity * cells_a + row + 1, :]
                value = value + line * columns[parity]
            if row == 0:
                value = value + walls[0, window, :]
            if row == cells_a - 1:
                value = value + walls[1, window, :]
            energy = energy + value * solved_ref[row, window, :]
            running = value if running is None else value + running
            running = running * factor_ref[row, window, :]
            source[row] = running
        nears = [solved_ref[0, window, :], solved_ref[cells_a - 1, window, :], None, running]
        total_ref[cells_a - 1, window, :] = nears[1] + running
        for row in range(cells_a - 2, -1, -1):
            running = source[row] + factor_ref[row, window, :] * running
            total_ref[row, window, :] = solved_ref[row, window, :] + running
        nears[2] = running
        for item in range(shares_count):
            for number, value in enumerate(nears):
                near_ref[step * shares_count + item, number] = value[
                    item * modes : (item + 1) * modes
                ]
        energy = jnp.sum(energy.reshape(block // 8, 8, length), axis=0)
        for part in range(length // 128):
            energy_ref[...] += energy[:, part * 128 : (part + 1) * 128]

    total, nears, energy_two = call(
        source_body,
        (blocks,),
        [SCALARS] + [RESIDENT] * 13,
        [RESIDENT] * 3,
        [field, kept(groups_x, 4, modes, length), kept(8, 128)],
        [
            pltpu.VMEM((TERMS, 128), F32),
            pltpu.VMEM((2, length, length), F32),
            pltpu.VMEM((2 * cells_a, length), F32),
            pltpu.VMEM((2 * cells_a, length), F32),
            pltpu.VMEM((depth, 2 * cells_a), F32),
            pltpu.VMEM((2 * cells_a, length), F32),
            pltpu.VMEM((2, depth, length), F32),
            pltpu.VMEM((cells_a, block, length), F32),
        ],
        10**9,
        "face_sources",
    )(
        place,
        shared,
        scales,
        unit_y,
        unit_z,
        unit_x,
        folded_high,
        folded_low,
        local_high,
        local_low,
        edge_rows,
        edge_columns,
        factors,
        solved,
    )

    gathered = lax.all_to_all(nears, "gx", 0, 0, tiled=True)

    def ghost_body(near_ref, green_ref, one_ref, two_ref, out_ref):
        first = [near_ref[s, 0] for s in range(groups_x)]
        last = [near_ref[s, 1] for s in range(groups_x)]
        other_first = [near_ref[s, 2] for s in range(groups_x)]
        other_last = [near_ref[s, 3] for s in range(groups_x)]
        energy_one = jnp.zeros((modes, length), F32)
        energy_two = jnp.zeros((modes, length), F32)
        for slab in range(groups_x):
            for side in range(2):
                value = jnp.zeros((modes, length), F32)
                other = jnp.zeros((modes, length), F32)
                neighbour = slab + (1 if side else -1)
                if 0 <= neighbour < groups_x:
                    value = (first if side else last)[neighbour]
                    other = (other_first if side else other_last)[neighbour]
                    base = (2 * slab + side) * ghosts
                    for s in range(groups_x):
                        near, far = green_ref[:, base + 2 * s, :], green_ref[:, base + 2 * s + 1, :]
                        value = value + near * first[s] + far * last[s]
                        other = other + near * other_first[s] + far * other_last[s]
                energy_one = energy_one + value * (last if side else first)[slab]
                energy_two = energy_two + value * (other_last if side else other_first)[slab]
                out_ref[slab, side * modes : (side + 1) * modes, :] = value + other
        top = lax.broadcasted_iota(jnp.int32, (8, 128), 0) == 0
        for number, (local_ref, value) in enumerate(((one_ref, energy_one), (two_ref, energy_two))):
            value = jnp.sum(value, axis=0, keepdims=True)
            line = value[:, 0:128]
            for part in range(1, length // 128):
                line = line + value[:, part * 128 : (part + 1) * 128]
            tile = local_ref[...] + jnp.where(top, line, 0.0)
            for slab in range(groups_x):
                out_ref[slab, 2 * modes : 2 * modes + 8, number * 128 : (number + 1) * 128] = tile

    height = 2 * modes + 8
    answers = call(
        ghost_body,
        (1,),
        [RESIDENT] * 4,
        RESIDENT,
        kept(groups_x, height, length),
        [],
        10**8,
        "ghost_values",
    )(gathered, green_table, energy_one, energy_two)
    returned = lax.all_to_all(answers, "gx", 0, 0, tiled=True)
    def back_body(number, total_ref, profile_ref, ghost_ref, weights, *rest):
        outs, energy_ref = rest[:groups_y], rest[groups_y]
        energy_ref[...] = jnp.sum(ghost_ref[:, 2 * modes : 2 * modes + 8, 0:256], axis=0)
        for step in range(blocks):
            back_block(total_ref, profile_ref, ghost_ref, outs, weights, step, number)

    def back_block(total_ref, profile_ref, ghost_ref, outs, weights, step, number):
        window = pl.ds(step * block, block)
        ghosts_here = [
            jnp.concatenate(
                [
                    ghost_ref[step * shares_count + item, side * modes : (side + 1) * modes, :]
                    for item in range(shares_count)
                ],
                axis=0,
            )
            for side in range(2)
        ]

        parts = []
        for item in range(number * part_tiles, (number + 1) * part_tiles):
            inner = []
            for row in range(item * pack, (item + 1) * pack):
                inner.append(
                    total_ref[row, window, :]
                    + profile_ref[row, window, :] * ghosts_here[0]
                    + profile_ref[cells_a - 1 - row, window, :] * ghosts_here[1]
                )
            parts.append(jnp.concatenate(inner, axis=1))
        result = triple(jnp.concatenate(parts, axis=0), weights[0], weights[1], NT)
        for shift in range(groups_y):
            for item in range(part_tiles):
                outs[shift][item, window, :] = result[
                    item * block : (item + 1) * block, shift * lanes : (shift + 1) * lanes
                ]

    arrived = []
    for number in range(halves):
        *parts, energy_tile = call(
            functools.partial(back_body, number),
            (1,),
            [RESIDENT] * 4,
            [RESIDENT] * (groups_y + 1),
            [piece] * groups_y + [kept(8, 256)],
            [],
            10**9,
            "second_back",
            limit=pair_limit,
        )(total, profile, returned, pairs)
        arrived.append(exchange(parts))
    arrived[-1][1], energy_tile = lax.optimization_barrier((arrived[-1][1], energy_tile))
    energy_tiles = exchange([energy_tile] * groups_y)

    norm = (2.0 / (length + 1)) ** 2

    def last_body(*refs):
        blocks_in = refs[:groups_y]
        table, out_ref = refs[groups_y], refs[-1]
        start = pl.program_id(0) * many
        values = [
            jnp.concatenate([part[start + item] for part in blocks_in], axis=0).T
            for item in range(many)
        ]
        result = triple(jnp.concatenate(values, axis=0), table[0], table[1], NN) * norm
        out_ref[...] = result.reshape(many * pack, cells_b, length)

    def final_body(*refs):
        tiles_in = refs[-2 - groups_y : -2]
        energy_ref = refs[-1]
        last_body(*refs[: groups_y + 1], refs[-2])

        @pl.when(pl.program_id(0) == 0)
        def _():
            value = tiles_in[0][...]
            for tile in tiles_in[1:]:
                value = value + tile[...]
            factor = spacing * norm
            first = jnp.sum(value[:, 0:128]) * factor
            energy_ref[0] = first
            energy_ref[1] = first + jnp.sum(value[:, 128:256]) * factor

    steps = part_tiles // many
    shape = jax.ShapeDtypeStruct(charge_density.shape, F32)
    base_specs = [RESIDENT] * (groups_y + 1)
    out_block = (many * pack, cells_b, length)
    potential = None
    for number in range(halves):
        inputs = [*arrived[number], table]
        specs, aliases = list(base_specs), None
        if number > 0:
            aliases = {len(inputs): 0}
            inputs.append(potential)
            specs.append(pl.BlockSpec(memory_space=pl.ANY))
        out_spec = pl.BlockSpec(out_block, lambda t, number=number: (t + number * steps, 0, 0))
        if number < halves - 1:
            potential = call(
                last_body, (steps,), specs, out_spec, shape, [], 10**9, "depth_back", aliases
            )(*inputs)
        else:
            potential, energies = call(
                final_body,
                (steps,),
                specs + [RESIDENT] * groups_y,
                [out_spec, SCALARS],
                [shape, jax.ShapeDtypeStruct((2,), F32)],
                [],
                10**9,
                "depth_back_last",
                aliases,
            )(*inputs, *energy_tiles)
    return potential, energies


def solution(mesh):
    placed = (P("gx", "gy", None),)
    return jax.shard_map(
        shards, mesh=mesh, in_specs=placed, out_specs=(P("gx", "gy", None), P()), check_vma=False
    )
```

```python
import functools
import math

import jax
import jax.numpy as jnp
import numpy as np
from jax import lax
from jax.experimental import pallas as pl
from jax.experimental.pallas import tpu as pltpu
from jax.sharding import PartitionSpec as P

ORDER = 16
COUNT = ORDER + 1
PAIRS = 256
FACE_ROWS = 16
TERMS = 384
outer_ratio = 1.1
radius_scale = math.sqrt(3.0) / 2.0
F32 = jnp.float32
BF16 = jnp.bfloat16
EXACT = lax.Precision.HIGHEST


NN = (((1,), (0,)), ((), ()))
NT = (((1,), (1,)), ((), ()))
TN = (((0,), (0,)), ((), ()))


def pair_list():
    return [(p, q) for p in range(COUNT) for q in range(COUNT - p)]


def term_list():
    terms = [(0, l, m) for m in range(COUNT) for l in range(m, COUNT)]
    terms += [(1, l, m) for m in range(1, COUNT) for l in range(m, COUNT)]
    return terms


def split_np(table):
    import ml_dtypes

    high = table.astype(np.float32).astype(ml_dtypes.bfloat16)
    low = (table - high.astype(np.float64)).astype(np.float32).astype(ml_dtypes.bfloat16)
    return high, low


def split(value):
    high = value.astype(BF16)
    return high, (value - high.astype(F32)).astype(BF16)


def mul(left, right, dims):
    return lax.dot_general(left, right, dims, preferred_element_type=F32)


def triple(left, high, low, dims):
    first, second = split(left)
    return mul(first, high, dims) + mul(first, low, dims) + mul(second, high, dims)


def inverted(value):
    guess = pl.reciprocal(value, approx=True)
    guess = guess * (2.0 - value * guess)
    return guess * (2.0 - value * guess)


def exact(left, right, dims):
    return lax.dot_general(left, right, dims, precision=EXACT, preferred_element_type=F32)


def solid_values(x, y, z):
    squared = x * x + y * y + z * z
    cosine, sine = {}, {}
    cosine[0, 0], sine[0, 0] = np.ones_like(x), np.zeros_like(x)
    for l in range(1, COUNT):
        scale = math.sqrt((2 * l - 1) / (2.0 * l)) if l > 1 else 1.0
        cosine[l, l] = scale * (x * cosine[l - 1, l - 1] - y * sine[l - 1, l - 1])
        sine[l, l] = scale * (x * sine[l - 1, l - 1] + y * cosine[l - 1, l - 1])
    for table in (cosine, sine):
        for m in range(COUNT):
            for l in range(m + 1, COUNT):
                older = table[l - 2, m] if l - 2 >= m else np.zeros_like(x)
                table[l, m] = (
                    (2 * l - 1) * z * table[l - 1, m]
                    - math.sqrt((l - 1) ** 2 - m * m) * squared * older
                ) / math.sqrt(l * l - m * m)
    return [(cosine, sine)[kind][l, m] for kind, l, m in term_list()]


@functools.cache
def constants(length):
    step = length + 1
    index = np.arange(length) + 1
    sine = np.sin(np.pi * ((index[:, None] * index[None, :]) % (2 * step)) / step)
    eigen = 4.0 * np.sin(np.pi * index / (2.0 * step)) ** 2
    cells = (np.arange(length) - (length - 1) / 2.0) / step
    legendre = np.stack(
        [np.polynomial.legendre.legval(2 * cells, np.eye(COUNT)[p]) for p in range(COUNT)]
    )
    hat = legendre @ sine
    edges = np.stack([sine[0] + sine[-1], sine[-1] - sine[0]])
    lookup = np.concatenate([hat, edges])
    columns = np.zeros((length, 128))
    columns[:, : COUNT + 2] = lookup.T
    spread = np.zeros((2, 128, PAIRS))
    own = np.zeros((2, 24, PAIRS))
    for spot, pair in enumerate(pair_list()):
        for kind in range(2):
            spread[kind, pair[kind], spot] = 1.0
            own[kind, pair[kind], spot] = 1.0
    nodes, weights = np.polynomial.legendre.leggauss(COUNT + 3)
    basis = np.stack([np.polynomial.legendre.legval(nodes, np.eye(COUNT)[p]) for p in range(COUNT)])
    project = basis * weights[None, :] * (2 * np.arange(COUNT)[:, None] + 1) / 2.0
    first, second = np.meshgrid(nodes / 2.0, nodes / 2.0, indexing="ij")
    half = np.full_like(first, 0.5)
    terms = term_list()
    scale = (1.0 / step) * (2.0 / step) ** 2
    maps = np.zeros((3, PAIRS, TERMS))
    places = [(half, first, second), (first, half, second), (first, second, half)]
    for face, place in enumerate(places):
        for column, values in enumerate(solid_values(*place)):
            degree = terms[column][1]
            expansion = project @ values @ project.T
            for spot, pair in enumerate(pair_list()):
                maps[face, spot, column] = scale * expansion[pair] / radius_scale**degree
    masks = np.zeros((3, 8, TERMS))
    for column, (kind, l, m) in enumerate(terms):
        masks[0, (m + kind) % 2, column] = 1.0
        masks[1, kind, column] = 1.0
        masks[2, (l - m) % 2, column] = 1.0
    folded = np.zeros((2, length // 2, length))
    parity = np.arange(length) % 2
    upper = 2.0 * sine[length // 2 :]
    folded[0] = upper * (parity == 0)
    folded[1] = upper * (parity == 1)
    return dict(
        sine=sine,
        eigen=eigen,
        cells=cells,
        legendre=legendre,
        columns=columns,
        spread=spread,
        own=own,
        edges=edges,
        maps=maps,
        masks=masks,
        folded=folded.reshape(length, length),
    )


def evaluation_scales():
    sector, running = [1.0], 1.0
    for l in range(1, COUNT):
        running *= math.sqrt((2 * l - 1) / (2.0 * l)) if l > 1 else 1.0
        sector.append(running)
    kappa, beta = {}, {}
    for m in range(COUNT):
        kappa[m, m] = sector[m]
        previous = 1.0
        for l in range(m + 1, COUNT):
            near = (2 * l - 1) / math.sqrt(l * l - m * m)
            far = math.sqrt((l - 1) ** 2 - m * m) / math.sqrt(l * l - m * m)
            kappa[l, m] = kappa[l - 1, m] * near
            beta[l, m] = far / (near * previous) if l >= m + 2 else 0.0
            previous = near
    scales = np.zeros((8, TERMS))
    for row, (_, l, m) in enumerate(term_list()):
        factor = 1.0 if m == 0 else 2.0
        weight = factor / (4.0 * math.pi * radius_scale * outer_ratio ** (l + 1))
        scales[:, row] = weight * kappa[l, m]
    return scales, beta


def evaluate(coef, unit_x, unit_y, unit_z):
    beta = evaluation_scales()[1]
    rows = {term: row for row, term in enumerate(term_list())}
    total = {}

    def add(key, value):
        total[key] = value if key not in total else total[key] + value

    cosine, sine = None, None
    for m in range(COUNT):
        if m == 1:
            cosine, sine = unit_x, unit_y
        elif m > 1:
            cosine, sine = unit_x * cosine - unit_y * sine, unit_x * sine + unit_y * cosine
        sums = {}
        older, newer = None, None
        for l in range(m, COUNT):
            if l == m:
                now = None
            elif l == m + 1:
                now = unit_z
            elif l == m + 2:
                now = unit_z * newer - beta[l, m]
            else:
                now = unit_z * newer - beta[l, m] * older
            for kind in range(1 if m == 0 else 2):
                row = rows[kind, l, m]
                weight = coef[row : row + 1, :]
                weight = jnp.broadcast_to(weight, unit_z.shape)
                term = weight if now is None else weight * now
                key = (kind, (l - m) % 2)
                sums[key] = term if key not in sums else sums[key] + term
            older, newer = newer, now
        for (kind, odd), value in sums.items():
            if m > 0:
                value = value * (cosine, sine)[kind]
            add((m % 2, kind, odd), value)
    return total


RESIDENT = pl.BlockSpec(memory_space=pltpu.VMEM)
SCALARS = pl.BlockSpec(memory_space=pltpu.SMEM)


def call(body, grid, in_specs, out_specs, out_shape, scratch, flops, aliases=None, limit=24):
    kernel = pl.pallas_call(
        body,
        grid=grid,
        in_specs=in_specs,
        out_specs=out_specs,
        out_shape=out_shape,
        scratch_shapes=scratch,
        input_output_aliases=aliases or {},
        cost_estimate=pl.CostEstimate(flops=flops, bytes_accessed=4 << 20, transcendentals=0),
        compiler_params=pltpu.CompilerParams(
            dimension_semantics=("arbitrary",) * len(grid), vmem_limit_bytes=limit << 20
        ),
    )

    def run(*args):
        placed = []
        for arg, spec in zip(args, in_specs):
            if spec is RESIDENT:
                arg = pltpu.with_memory_space_constraint(arg, pltpu.VMEM)
            elif spec.block_shape is not None:
                arg = pltpu.with_memory_space_constraint(arg, pltpu.HBM)
            placed.append(arg)
        return kernel(*placed)

    return run


def kept(*shape):
    return pltpu.VMEM(shape, F32)


def shards(charge_density):
    cells_a, cells_b, length = charge_density.shape
    groups_x, groups_y = lax.axis_size("gx"), lax.axis_size("gy")
    devices = groups_x * groups_y
    index_x, index_y = lax.axis_index("gx"), lax.axis_index("gy")
    tabs = constants(length)
    spacing = 1.0 / (length + 1)
    pack = max(1, 128 // cells_b)
    lanes = pack * cells_b
    wide = pack * length
    tiles = cells_a // pack
    depth = cells_b
    block = min(64, depth)
    blocks = depth // block
    modes = depth // groups_x
    ghosts = 2 * groups_x
    functions = COUNT + 2
    place = jnp.stack([index_x, index_y]).astype(jnp.int32)

    def const(name):
        return jnp.asarray(tabs[name].astype(np.float32))

    sine_high, sine_low = (jnp.asarray(t) for t in split_np(tabs["sine"]))
    sine_high = sine_high.reshape(groups_y, cells_b, length)
    sine_low = sine_low.reshape(groups_y, cells_b, length)
    parts_in = tiles // 4 if tiles % 4 == 0 else tiles
    uneven = parts_in < tiles
    going = [parts_in, 3 * parts_in] if uneven else [tiles]
    coming = [parts_in, 2 * parts_in, parts_in] if uneven else [tiles]

    def starts_of(portions):
        return [sum(portions[:number]) for number in range(len(portions))]

    pair_limit = 24 if wide <= 512 else 44

    def fill_pairs(weights, high_ref, low_ref, index_y):
        weights[...] = jnp.zeros_like(weights)
        for shift in range(groups_y):
            peer = index_y ^ shift
            for item in range(pack):
                rows = pl.ds(shift * lanes + item * cells_b, cells_b)
                weights[0, rows, item * length : (item + 1) * length] = high_ref[peer]
                weights[1, rows, item * length : (item + 1) * length] = low_ref[peer]

    many = min(4, parts_in)

    def depth_body(place_ref, rho_ref, high_ref, low_ref, *rest):
        outs, table = rest[:groups_y], rest[groups_y]

        @pl.when(pl.program_id(0) == 0)
        def _():
            for shift in range(groups_y):
                peer = place_ref[1] ^ shift
                table[0, pl.ds(shift * cells_b, cells_b), :] = high_ref[peer]
                table[1, pl.ds(shift * cells_b, cells_b), :] = low_ref[peer]

        value = rho_ref[...].reshape(many * lanes, length)
        high, low = split(value)
        result = mul(table[0], high, NT) + mul(table[1], high, NT) + mul(table[0], low, NT)
        start = pl.program_id(0) * many
        for shift in range(groups_y):
            for item in range(many):
                outs[shift][start + item] = result[
                    shift * cells_b : (shift + 1) * cells_b, item * lanes : (item + 1) * lanes
                ]

    def pieces_of(count):
        return [kept(count, depth, lanes)] * groups_y

    table_spec = pl.BlockSpec((groups_y, cells_b, length), lambda t: (0, 0, 0))

    def depth_transform(number):
        steps, first = going[number] // many, starts_of(going)[number] // many
        return call(
            depth_body,
            (steps,),
            [
                SCALARS,
                pl.BlockSpec((many * pack, cells_b, length), lambda t: (t + first, 0, 0)),
                table_spec,
                table_spec,
            ],
            [RESIDENT] * groups_y,
            pieces_of(going[number]),
            [pltpu.VMEM((2, length, length), BF16)],
            10**9,
        )(
            place,
            charge_density,
            sine_high,
            sine_low,
        )

    def exchange(parts):
        received = [parts[0]]
        for shift in range(1, groups_y):
            ring = [(source, source ^ shift) for source in range(groups_y)]
            received.append(lax.ppermute(parts[shift], "gy", ring))
        return received

    received = []
    for number in range(len(going)):
        parts = depth_transform(number)
        received.append(exchange(parts))

    half = length // 2
    sine64 = tabs["sine"]
    scale = 2.0 / (length + 1)
    hat_all = scale * np.concatenate([tabs["legendre"] @ sine64, tabs["edges"]])
    hat_pad = -(-functions // 8) * 8
    hat_all = np.concatenate([hat_all, np.zeros((hat_pad - functions, length))])
    blank = np.zeros((1, length))
    lines = np.concatenate([blank, sine64, blank])
    spots = []
    for slab in range(groups_x):
        spots += [slab * cells_a, (slab + 1) * cells_a + 1]
    green_lines = lines[spots]
    green = (scale * green_lines[:, None, :] * green_lines[None, :, :]).reshape(-1, length)
    eigen_column = np.broadcast_to(tabs["eigen"][:, None], (length, length))
    eigen_row = np.broadcast_to(tabs["eigen"][None, :], (8, length))
    cell_column = np.broadcast_to(tabs["cells"][:, None], (length, half))
    cell_row = np.broadcast_to(tabs["cells"][None, half:], (8, half))

    def put(table):
        return jnp.asarray(np.ascontiguousarray(table).astype(np.float32))

    def prepare_body(
        place_ref,
        column_ref,
        row_ref,
        line_ref,
        hat_ref,
        green_high_ref,
        green_low_ref,
        cell_column_ref,
        cell_row_ref,
        sine_high_ref,
        sine_low_ref,
        factor_ref,
        profile_ref,
        probe_ref,
        green_ref,
        unit_ref,
        pair_ref,
        table_ref,
        values,
        probe_high,
        probe_low,
    ):
        index_x, index_y = place_ref[0], place_ref[1]
        fill_pairs(pair_ref, sine_high_ref, sine_low_ref, index_y)
        for shift in range(groups_y):
            peer = index_y ^ shift
            table_ref[0, pl.ds(shift * cells_b, cells_b), :] = sine_high_ref[peer]
            table_ref[1, pl.ds(shift * cells_b, cells_b), :] = sine_low_ref[peer]
        own = pl.ds(pl.multiple_of(index_y * depth, depth), depth)
        values[...] = column_ref[own, :] + row_ref[0:1, :]
        value = values[...] + 2.0
        factor = inverted(value)
        running = factor
        factor_ref[0] = factor
        profile_ref[0] = running
        for row in range(1, cells_a):
            factor = inverted(value - factor)
            running = running * factor
            factor_ref[row] = factor
            profile_ref[row] = running
        for row in range(cells_a - 2, -1, -1):
            running = profile_ref[row] + factor_ref[row] * running
            profile_ref[row] = running
        for side in range(2):
            spot = index_x * cells_a + side * (cells_a + 1)
            table = line_ref[pl.ds(spot, 1), :] * hat_ref[...]
            high, low = split(table)
            probe_high[side * hat_pad : (side + 1) * hat_pad] = high
            probe_low[side * hat_pad : (side + 1) * hat_pad] = low

        def inverse_of(spot):
            return split(inverted(column_ref[...] + values[pl.ds(spot, 1), :]))

        def probe_step(number, carry):
            high, low = inverse_of(number)
            answer = (
                mul(probe_high[...], high, NN)
                + mul(probe_low[...], high, NN)
                + mul(probe_high[...], low, NN)
            )
            rows = pl.ds(pl.multiple_of(number * 2 * hat_pad, 8), 2 * hat_pad)
            for part in range(length // 128):
                probe_ref[part, rows, :] = answer[:, part * 128 : (part + 1) * 128]
            return carry

        lax.fori_loop(0, depth, probe_step, 0, unroll=4)

        def green_step(number, carry):
            high, low = inverse_of(index_x * modes + number)
            answer = (
                mul(green_high_ref[...], high, NN)
                + mul(green_low_ref[...], high, NN)
                + mul(green_high_ref[...], low, NN)
            )
            green_ref[pl.ds(number, 1)] = answer[None]
            return carry

        lax.fori_loop(0, modes, green_step, 0, unroll=min(2, modes))
        here = pl.ds(pl.multiple_of(index_x * cells_a, cells_a), cells_a)
        middle = jnp.full((8, half), 0.5, F32)[0:1]
        along = cell_row_ref[0:1, :]
        for begin, count, first, second, third in (
            (0, cells_a, cell_column_ref[here, :], middle, along),
            (cells_a, cells_a, cell_column_ref[here, :], along, middle),
            (2 * cells_a, half, middle, cell_column_ref[half:, :], along),
        ):
            inverse = 1.0 / jnp.sqrt(first * first + second * second + third * third)
            unit_ref[0, begin : begin + count] = first * inverse
            unit_ref[1, begin : begin + count] = second * inverse
            unit_ref[2, begin : begin + count] = third * inverse

    field = kept(cells_a, depth, length)
    green_high, green_low = (jnp.asarray(t) for t in split_np(green))
    inputs = (
        put(eigen_column),
        put(eigen_row),
        put(lines),
        put(hat_all),
        green_high,
        green_low,
        put(cell_column),
        put(cell_row),
        sine_high,
        sine_low,
    )

    def block_of(array):
        zeros = (0,) * array.ndim
        return pl.BlockSpec(array.shape, lambda k: zeros)

    tables = call(
        prepare_body,
        (1,),
        [SCALARS] + [block_of(array) for array in inputs],
        [RESIDENT] * 7,
        [
            field,
            field,
            kept(length // 128, depth * 2 * hat_pad, 128),
            kept(modes, ghosts * ghosts, length),
            kept(3, 2 * cells_a + half, half),
            pltpu.VMEM((2, groups_y * lanes, wide), BF16),
            pltpu.VMEM((2, length, length), BF16),
        ],
        [
            pltpu.VMEM((depth, length), F32),
            pltpu.VMEM((2 * hat_pad, length), BF16),
            pltpu.VMEM((2 * hat_pad, length), BF16),
        ],
        10**10,
        limit=pair_limit,
    )(place, *inputs)
    legendre = put(tabs["legendre"])
    edge_rows = put(np.concatenate([tabs["edges"], np.zeros((6, length))]))
    edge_columns = put(np.broadcast_to(tabs["edges"][:, :, None], (2, length, 128)))
    column_high, column_low = (jnp.asarray(t) for t in split_np(tabs["columns"]))
    lookup = np.zeros((groups_y, 24, depth))
    lookup[:, : COUNT + 2] = (
        tabs["columns"][:, : COUNT + 2].T.reshape(COUNT + 2, groups_y, depth).transpose(1, 0, 2)
    )
    lookup = lookup.reshape(groups_y, 24, blocks, block).transpose(0, 2, 1, 3)
    lookup_high, lookup_low = (jnp.asarray(t) for t in split_np(lookup))
    spread = jnp.asarray(tabs["spread"].astype(np.float32)).astype(BF16)
    map_high, map_low = (jnp.asarray(t) for t in split_np(tabs["maps"]))
    factors, profile, probe_table, green_table, units, pairs, table = tables

    def second_body(*refs):
        blocks_in = refs[:groups_y]
        weights, out_ref = refs[groups_y:]
        part_tiles = out_ref.shape[0] // pack
        for start in range(0, depth, block):
            value = jnp.concatenate(
                [
                    part[:, start : start + block, :].reshape(part_tiles * block, lanes)
                    for part in blocks_in
                ],
                axis=1,
            )
            result = triple(value, weights[0], weights[1], NN) * (spacing * spacing)
            for item in range(part_tiles):
                for inner in range(pack):
                    out_ref[item * pack + inner, start : start + block, :] = result[
                        item * block : (item + 1) * block, inner * length : (inner + 1) * length
                    ]

    sources = []
    for number, parts in enumerate(received):
        sources.append(
            call(
                second_body,
                (1,),
                [RESIDENT] * (groups_y + 1),
                RESIDENT,
                kept(going[number] * pack, depth, length),
                [],
                10**9,
                limit=pair_limit,
            )(*parts, pairs)
        )

    rows_now = min(32, block)

    def solve_body(place_ref, leg_ref, *refs):
        given = refs[: len(going)]
        (
            factor_ref,
            probe_ref,
            column_high_ref,
            column_low_ref,
            lookup_high_ref,
            lookup_low_ref,
            spread_ref,
            own_ref,
            map_high_ref,
            map_low_ref,
            mask_ref,
            field_ref,
            moment_ref,
            energy_ref,
            tensor,
        ) = refs[len(going) :]
        index_x, index_y = place_ref[0], place_ref[1]
        begin = jnp.where(index_x == 0, 1.0, 0.0)
        finish = jnp.where(index_x == groups_x - 1, 1.0, 0.0)
        step = pl.program_id(0)
        base = pl.multiple_of(step * block, block)
        window = pl.ds(base, block)

        @pl.when(step == 0)
        def _():
            tensor[...] = jnp.zeros_like(tensor)
            energy_ref[...] = jnp.zeros_like(energy_ref)

        def source(row, begin_row):
            starts = starts_of(going)
            number = max(n for n in range(len(going)) if starts[n] * pack <= row)
            return given[number][row - starts[number] * pack, pl.ds(begin_row, rows_now), :]

        def eliminate(begin_row):
            strip = pl.ds(begin_row, rows_now)
            running = source(0, begin_row) * factor_ref[0, strip, :]
            field_ref[0, strip, :] = running
            for row in range(1, cells_a):
                running = (source(row, begin_row) + running) * factor_ref[row, strip, :]
                field_ref[row, strip, :] = running
            energy = source(cells_a - 1, begin_row) * running
            for row in range(cells_a - 2, -1, -1):
                running = field_ref[row, strip, :] + factor_ref[row, strip, :] * running
                field_ref[row, strip, :] = running
                energy = energy + source(row, begin_row) * running
            energy = jnp.sum(energy.reshape(rows_now // 8, 8, length), axis=0)
            for part in range(length // 128):
                energy_ref[...] += energy[:, part * 128 : (part + 1) * 128]

        for offset in range(0, block, rows_now):
            eliminate(pl.multiple_of(base + offset, rows_now))
        first, last = field_ref[0, window, :], field_ref[cells_a - 1, window, :]
        table_high, table_low = column_high_ref[...], column_low_ref[...]
        rows_high = lookup_high_ref[index_y, step]
        rows_low = lookup_low_ref[index_y, step]

        def contract(stack, count):
            answer = triple(stack, table_high, table_low, NN)
            upper, lower = split(answer)
            outs = []
            for item in range(count):
                high = upper[item * block : (item + 1) * block]
                low = lower[item * block : (item + 1) * block]
                outs.append(
                    mul(rows_high, high, NN) + mul(rows_low, high, NN) + mul(rows_high, low, NN)
                )
            return outs

        many_rows = min(16, cells_a)
        for start in range(0, cells_a, many_rows):
            stack = field_ref[start : start + many_rows, window, :].reshape(
                many_rows * block, length
            )
            outs = contract(stack, many_rows)
            for item in range(COUNT):
                value = tensor[item]
                for inner, out in enumerate(outs):
                    value = value + leg_ref[item, index_x * cells_a + start + inner] * out
                tensor[item] = value
            if start == 0:
                tensor[COUNT] += begin * outs[0]
                tensor[COUNT + 1] -= begin * outs[0]
            if start + many_rows == cells_a:
                tensor[COUNT] += finish * outs[-1]
                tensor[COUNT + 1] += finish * outs[-1]

        def probe_row(item):
            rows = pl.ds(base * 2 * hat_pad + item, block, stride=2 * hat_pad)
            return jnp.concatenate(
                [probe_ref[part, rows, :] for part in range(length // 128)], axis=1
            )

        group = 10
        for start in range(0, functions, group):
            items = range(start, min(start + group, functions))
            stack = jnp.concatenate(
                [
                    probe_row(item) * first + probe_row(hat_pad + item) * last
                    for item in items
                ],
                axis=0,
            )
            for item, out in zip(items, contract(stack, len(items))):
                tensor[item] += out

        @pl.when(step == blocks - 1)
        def _():
            rows = lax.broadcasted_iota(jnp.int32, (8, PAIRS), 0)

            def flatten(matrix, kind):
                high, low = split(matrix)
                answer = mul(high, spread_ref[kind], NN) + mul(low, spread_ref[kind], NN)
                return jnp.sum(answer * own_ref[1 - kind], axis=0, keepdims=True)

            moments = jnp.zeros((8, TERMS), F32)
            for face in range(3):
                stack = jnp.zeros((8, PAIRS), F32)
                for parity in range(2):
                    if face == 0:
                        value = flatten(tensor[COUNT + parity], 0)
                    elif face == 1:
                        value = jnp.zeros((1, PAIRS), F32)
                        for item in range(COUNT):
                            column = tensor[item, :, COUNT + parity : COUNT + parity + 1]
                            chosen = own_ref[0, item : item + 1, :] * own_ref[1]
                            value = value + jnp.sum(column * chosen, axis=0, keepdims=True)
                    else:
                        matrix = jnp.concatenate(
                            [
                                tensor[item, COUNT + parity : COUNT + parity + 1, :]
                                for item in range(COUNT)
                            ]
                            + [jnp.zeros((24 - COUNT, 128), F32)],
                            axis=0,
                        )
                        high, low = split(matrix)
                        answer = mul(high, spread_ref[1], NN) + mul(low, spread_ref[1], NN)
                        value = jnp.sum(answer * own_ref[0], axis=0, keepdims=True)
                    stack = jnp.where(rows == parity, value, stack)
                moments = moments + triple(stack, map_high_ref[face], map_low_ref[face], NN) * (
                    mask_ref[face]
                )
            moments = jnp.sum(moments, axis=0, keepdims=True)
            moment_ref[...] = jnp.broadcast_to(moments[None], moment_ref.shape)

    solved, moments, energy_one = call(
        solve_body,
        (blocks,),
        [SCALARS] * 2 + [RESIDENT] * (len(going) + 11),
        [RESIDENT] * 3,
        [field, kept(devices, 1, TERMS), kept(8, 128)],
        [
            pltpu.VMEM((24, 24, 128), F32),
        ],
        10**9,
    )(
        place,
        legendre,
        *sources,
        factors,
        probe_table,
        column_high,
        column_low,
        lookup_high,
        lookup_low,
        spread,
        const("own"),
        map_high,
        map_low,
        const("masks"),
    )
    shared = lax.all_to_all(moments, ("gx", "gy"), 0, 0, tiled=True)

    scales = jnp.asarray(evaluation_scales()[0].astype(np.float32))
    folded_high, folded_low = (jnp.asarray(t) for t in split_np(tabs["folded"]))
    local_high, local_low = (
        jnp.asarray(np.ascontiguousarray(t.T).reshape(groups_y, depth, length))
        for t in split_np(tabs["folded"])
    )
    strip = min(32, cells_a)
    shares_count = block // modes
    face_rows = min(FACE_ROWS, block)

    def source_body(
        place_ref,
        share_ref,
        scale_ref,
        unit_ref,
        folded_high_ref,
        folded_low_ref,
        local_high_ref,
        local_low_ref,
        row_ref,
        column_ref,
        factor_ref,
        solved_ref,
        total_ref,
        near_ref,
        energy_ref,
        coef,
        values,
        plane_x,
        plane_y,
        plane_z,
        lines_y,
        lines_z,
        walls,
    ):
        index_x, index_y = place_ref[0], place_ref[1]
        begin = jnp.where(index_x == 0, 1.0, 0.0)
        finish = jnp.where(index_x == groups_x - 1, 1.0, 0.0)

        step = pl.program_id(0)
        window = pl.ds(pl.multiple_of(step * block, block), block)

        @pl.when(step == 0)
        def _():
            ones = jnp.full((8, 128), 0.125, F32)
            shares = jnp.sum(share_ref[...], axis=0) * scale_ref[...]
            coef[...] = exact(shares, ones, TN)
            energy_ref[...] = jnp.zeros_like(energy_ref)

            def one_strip(number, carry):
                window = pl.ds(pl.multiple_of(number * strip, strip), strip)
                classes = evaluate(
                    coef, unit_ref[0, window, :], unit_ref[1, window, :], unit_ref[2, window, :]
                )
                for (azimuth, kind, odd), value in classes.items():
                    values[azimuth * 4 + kind * 2 + odd, window, :] = value
                return carry

            lax.fori_loop(0, (2 * cells_a + half) // strip, one_strip, 0)
            for kind in range(2):
                for odd in range(2):
                    for start, target, row, column in (
                        (0, plane_y, kind, odd),
                        (cells_a, plane_z, odd, kind),
                    ):
                        target[
                            row * cells_a : (row + 1) * cells_a, column * half : (column + 1) * half
                        ] = (
                            values[kind * 2 + odd, start : start + cells_a, :]
                            + values[4 + kind * 2 + odd, start : start + cells_a, :]
                        )
                    even, other = (
                        values[parity * 4 + kind * 2 + odd, 2 * cells_a :, :]
                        for parity in (kind, 1 - kind)
                    )
                    plane_x[
                        kind * half : (kind + 1) * half, odd * half : (odd + 1) * half
                    ] = even + (finish - begin) * other
            folded_tables = folded_high_ref[...], folded_low_ref[...]
            local_tables = local_high_ref[index_y], local_low_ref[index_y]

            def across(plane):
                upper, lower = split(plane)
                high, low = local_tables
                return mul(high, upper, NT) + mul(low, upper, NT) + mul(high, lower, NT)

            lines_z[...] = triple(plane_z[...], *folded_tables, NN)
            lines_y[...] = across(plane_y[...])
            wall = triple(across(plane_x[...]), *folded_tables, NN)
            walls[0] = begin * wall
            walls[1] = finish * wall


        def eliminate(offset):
            begin_row = pl.multiple_of(step * block + offset, face_rows)
            window = pl.ds(begin_row, face_rows)
            here = pl.ds(pl.multiple_of(index_y * depth + begin_row, face_rows), face_rows)
            columns = [
                jnp.concatenate([column_ref[parity, here, :]] * (length // 128), axis=1)
                for parity in range(2)
            ]
            line_block = lines_y[window, :]
            energy = jnp.zeros((face_rows, length), F32)
            running = None
            for row in range(cells_a):
                value = None
                for parity in range(2):
                    spot = parity * cells_a + row
                    term = line_block[:, spot : spot + 1] * row_ref[parity : parity + 1, :]
                    value = term if value is None else value + term
                    value = value + lines_z[spot : spot + 1, :] * columns[parity]
                if row == 0:
                    value = value + walls[0, window, :]
                if row == cells_a - 1:
                    value = value + walls[1, window, :]
                energy = energy + value * solved_ref[row, window, :]
                running = value if running is None else value + running
                running = running * factor_ref[row, window, :]
                total_ref[row, window, :] = running
            nears = [solved_ref[0, window, :], solved_ref[cells_a - 1, window, :], None, running]
            total_ref[cells_a - 1, window, :] = nears[1] + running
            for row in range(cells_a - 2, -1, -1):
                running = total_ref[row, window, :] + factor_ref[row, window, :] * running
                total_ref[row, window, :] = solved_ref[row, window, :] + running
            nears[2] = running
            for item in range(face_rows // modes):
                for number, value in enumerate(nears):
                    near_ref[(step * block + offset) // modes + item, number] = value[
                        item * modes : (item + 1) * modes
                    ]
            energy = jnp.sum(energy.reshape(face_rows // 8, 8, length), axis=0)
            for part in range(length // 128):
                energy_ref[...] += energy[:, part * 128 : (part + 1) * 128]

        for offset in range(0, block, face_rows):
            eliminate(offset)

    total, nears, energy_two = call(
        source_body,
        (blocks,),
        [SCALARS] + [RESIDENT] * 11,
        [RESIDENT] * 3,
        [field, kept(groups_x, 4, modes, length), kept(8, 128)],
        [
            pltpu.VMEM((TERMS, 128), F32),
            kept(8, 2 * cells_a + half, half),
            pltpu.VMEM((length, length), F32),
            pltpu.VMEM((2 * cells_a, length), F32),
            pltpu.VMEM((2 * cells_a, length), F32),
            pltpu.VMEM((depth, 2 * cells_a), F32),
            pltpu.VMEM((2 * cells_a, length), F32),
            pltpu.VMEM((2, depth, length), F32),
        ],
        10**9,
    )(
        place,
        shared,
        scales,
        units,
        folded_high,
        folded_low,
        local_high,
        local_low,
        edge_rows,
        edge_columns,
        factors,
        solved,
    )

    gathered = lax.all_to_all(nears, "gx", 0, 0, tiled=True)

    def ghost_body(near_ref, green_ref, one_ref, two_ref, out_ref):
        first = [near_ref[s, 0] for s in range(groups_x)]
        last = [near_ref[s, 1] for s in range(groups_x)]
        other_first = [near_ref[s, 2] for s in range(groups_x)]
        other_last = [near_ref[s, 3] for s in range(groups_x)]
        energy_one = jnp.zeros((modes, length), F32)
        energy_two = jnp.zeros((modes, length), F32)
        for slab in range(groups_x):
            for side in range(2):
                value = jnp.zeros((modes, length), F32)
                other = jnp.zeros((modes, length), F32)
                neighbour = slab + (1 if side else -1)
                if 0 <= neighbour < groups_x:
                    value = (first if side else last)[neighbour]
                    other = (other_first if side else other_last)[neighbour]
                    base = (2 * slab + side) * ghosts
                    for s in range(groups_x):
                        near, far = green_ref[:, base + 2 * s, :], green_ref[:, base + 2 * s + 1, :]
                        value = value + near * first[s] + far * last[s]
                        other = other + near * other_first[s] + far * other_last[s]
                energy_one = energy_one + value * (last if side else first)[slab]
                energy_two = energy_two + value * (other_last if side else other_first)[slab]
                out_ref[slab, side * modes : (side + 1) * modes, :] = value + other
        top = lax.broadcasted_iota(jnp.int32, (8, 128), 0) == 0
        for number, (local_ref, value) in enumerate(((one_ref, energy_one), (two_ref, energy_two))):
            value = jnp.sum(value, axis=0, keepdims=True)
            line = value[:, 0:128]
            for part in range(1, length // 128):
                line = line + value[:, part * 128 : (part + 1) * 128]
            tile = local_ref[...] + jnp.where(top, line, 0.0)
            for slab in range(groups_x):
                out_ref[slab, 2 * modes : 2 * modes + 8, number * 128 : (number + 1) * 128] = tile

    height = 2 * modes + 8
    answers = call(
        ghost_body, (1,), [RESIDENT] * 4, RESIDENT, kept(groups_x, height, length), [], 10**8
    )(gathered, green_table, energy_one, energy_two)
    returned = lax.all_to_all(answers, "gx", 0, 0, tiled=True)

    def back_body(number, total_ref, profile_ref, ghost_ref, weights, *rest):
        outs, energy_ref = rest[:groups_y], rest[groups_y]
        energy_ref[...] = jnp.sum(ghost_ref[:, 2 * modes : 2 * modes + 8, 0:256], axis=0)
        for step in range(blocks):
            back_block(total_ref, profile_ref, ghost_ref, outs, weights, step, number)

    def back_block(total_ref, profile_ref, ghost_ref, outs, weights, step, number):
        window = pl.ds(step * block, block)
        ghosts_here = [
            jnp.concatenate(
                [
                    ghost_ref[step * shares_count + item, side * modes : (side + 1) * modes, :]
                    for item in range(shares_count)
                ],
                axis=0,
            )
            for side in range(2)
        ]

        parts = []
        for item in range(starts_of(coming)[number], starts_of(coming)[number] + coming[number]):
            inner = []
            for row in range(item * pack, (item + 1) * pack):
                inner.append(
                    total_ref[row, window, :]
                    + profile_ref[row, window, :] * ghosts_here[0]
                    + profile_ref[cells_a - 1 - row, window, :] * ghosts_here[1]
                )
            parts.append(jnp.concatenate(inner, axis=1))
        result = triple(jnp.concatenate(parts, axis=0), weights[0], weights[1], NT)
        for shift in range(groups_y):
            for item in range(coming[number]):
                outs[shift][item, window, :] = result[
                    item * block : (item + 1) * block, shift * lanes : (shift + 1) * lanes
                ]

    arrived = []
    for number in range(len(coming)):
        *parts, tile_now = call(
            functools.partial(back_body, number),
            (1,),
            [RESIDENT] * 4,
            [RESIDENT] * (groups_y + 1),
            pieces_of(coming[number]) + [kept(8, 256)],
            [],
            10**9,
            limit=pair_limit,
        )(total, profile, returned, pairs)
        energy_tile = tile_now if number == 0 else energy_tile
        arrived.append(exchange(parts))
    energy_tiles = exchange([energy_tile] * groups_y)

    norm = (2.0 / (length + 1)) ** 2

    def last_body(*refs):
        blocks_in = refs[:groups_y]
        table, out_ref = refs[groups_y], refs[-1]
        start = pl.program_id(0) * many
        values = [
            jnp.concatenate([part[start + item] for part in blocks_in], axis=0).T
            for item in range(many)
        ]
        result = triple(jnp.concatenate(values, axis=0), table[0], table[1], NN) * norm
        out_ref[...] = result.reshape(many * pack, cells_b, length)

    def final_body(*refs):
        tiles_in = refs[-2 - groups_y : -2]
        energy_ref = refs[-1]
        last_body(*refs[: groups_y + 1], refs[-2])

        @pl.when(pl.program_id(0) == 0)
        def _():
            value = tiles_in[0][...]
            for tile in tiles_in[1:]:
                value = value + tile[...]
            factor = spacing * norm
            first = jnp.sum(value[:, 0:128]) * factor
            energy_ref[0] = first
            energy_ref[1] = first + jnp.sum(value[:, 128:256]) * factor

    shape = jax.ShapeDtypeStruct(charge_density.shape, F32)
    base_specs = [RESIDENT] * (groups_y + 1)
    out_block = (many * pack, cells_b, length)
    potential = None
    for number in range(len(coming)):
        steps, first = coming[number] // many, starts_of(coming)[number] // many
        inputs = [*arrived[number], table]
        specs, aliases = list(base_specs), None
        if number > 0:
            aliases = {len(inputs): 0}
            inputs.append(potential)
            specs.append(pl.BlockSpec(memory_space=pl.ANY))
        out_spec = pl.BlockSpec(out_block, lambda t, first=first: (t + first, 0, 0))
        if number < len(coming) - 1:
            potential = call(
                last_body, (steps,), specs, out_spec, shape, [], 10**9, aliases
            )(*inputs)
        else:
            potential, energies = call(
                final_body,
                (steps,),
                specs + [RESIDENT] * groups_y,
                [out_spec, SCALARS],
                [shape, jax.ShapeDtypeStruct((2,), F32)],
                [],
                10**9,
                aliases,
            )(*inputs, *energy_tiles)
    return potential, energies


def solution(mesh):
    placed = (P("gx", "gy", None),)
    return jax.shard_map(
        shards, mesh=mesh, in_specs=placed, out_specs=(P("gx", "gy", None), P()), check_vma=False
    )
```

```python
import functools
import math

import jax
import jax.numpy as jnp
import numpy as np
from jax import lax
from jax.experimental import pallas as pl
from jax.experimental.pallas import tpu as pltpu
from jax.sharding import PartitionSpec as P

ORDER = 16
COUNT = ORDER + 1
PAIRS = 256
NEWTON = 1
FACE_ROWS = 16
TERMS = 384
outer_ratio = 1.1
radius_scale = math.sqrt(3.0) / 2.0
F32 = jnp.float32
BF16 = jnp.bfloat16
EXACT = lax.Precision.HIGHEST


NN = (((1,), (0,)), ((), ()))
NT = (((1,), (1,)), ((), ()))
TN = (((0,), (0,)), ((), ()))


def pair_list():
    return [(p, q) for p in range(COUNT) for q in range(COUNT - p)]


def term_list():
    terms = [(0, l, m) for m in range(COUNT) for l in range(m, COUNT)]
    terms += [(1, l, m) for m in range(1, COUNT) for l in range(m, COUNT)]
    return terms


def split_np(table):
    import ml_dtypes

    high = table.astype(np.float32).astype(ml_dtypes.bfloat16)
    low = (table - high.astype(np.float64)).astype(np.float32).astype(ml_dtypes.bfloat16)
    return high, low


def split(value):
    high = value.astype(BF16)
    return high, (value - high.astype(F32)).astype(BF16)


def mul(left, right, dims):
    return lax.dot_general(left, right, dims, preferred_element_type=F32)


def triple(left, high, low, dims):
    first, second = split(left)
    return mul(first, high, dims) + mul(first, low, dims) + mul(second, high, dims)


def inverted(value):
    guess = pl.reciprocal(value, approx=True)
    for _ in range(NEWTON):
        guess = guess * (2.0 - value * guess)
    return guess


def exact(left, right, dims):
    return lax.dot_general(left, right, dims, precision=EXACT, preferred_element_type=F32)


def solid_values(x, y, z):
    squared = x * x + y * y + z * z
    cosine, sine = {}, {}
    cosine[0, 0], sine[0, 0] = np.ones_like(x), np.zeros_like(x)
    for l in range(1, COUNT):
        scale = math.sqrt((2 * l - 1) / (2.0 * l)) if l > 1 else 1.0
        cosine[l, l] = scale * (x * cosine[l - 1, l - 1] - y * sine[l - 1, l - 1])
        sine[l, l] = scale * (x * sine[l - 1, l - 1] + y * cosine[l - 1, l - 1])
    for table in (cosine, sine):
        for m in range(COUNT):
            for l in range(m + 1, COUNT):
                older = table[l - 2, m] if l - 2 >= m else np.zeros_like(x)
                table[l, m] = (
                    (2 * l - 1) * z * table[l - 1, m]
                    - math.sqrt((l - 1) ** 2 - m * m) * squared * older
                ) / math.sqrt(l * l - m * m)
    return [(cosine, sine)[kind][l, m] for kind, l, m in term_list()]


@functools.cache
def constants(length):
    step = length + 1
    index = np.arange(length) + 1
    sine = np.sin(np.pi * ((index[:, None] * index[None, :]) % (2 * step)) / step)
    eigen = 4.0 * np.sin(np.pi * index / (2.0 * step)) ** 2
    cells = (np.arange(length) - (length - 1) / 2.0) / step
    legendre = np.stack(
        [np.polynomial.legendre.legval(2 * cells, np.eye(COUNT)[p]) for p in range(COUNT)]
    )
    hat = legendre @ sine
    edges = np.stack([sine[0] + sine[-1], sine[-1] - sine[0]])
    lookup = np.concatenate([hat, edges])
    columns = np.zeros((length, 128))
    columns[:, : COUNT + 2] = lookup.T
    spread = np.zeros((2, 128, PAIRS))
    own = np.zeros((2, 24, PAIRS))
    for spot, pair in enumerate(pair_list()):
        for kind in range(2):
            spread[kind, pair[kind], spot] = 1.0
            own[kind, pair[kind], spot] = 1.0
    nodes, weights = np.polynomial.legendre.leggauss(COUNT + 3)
    basis = np.stack([np.polynomial.legendre.legval(nodes, np.eye(COUNT)[p]) for p in range(COUNT)])
    project = basis * weights[None, :] * (2 * np.arange(COUNT)[:, None] + 1) / 2.0
    first, second = np.meshgrid(nodes / 2.0, nodes / 2.0, indexing="ij")
    half = np.full_like(first, 0.5)
    terms = term_list()
    scale = (1.0 / step) * (2.0 / step) ** 2
    maps = np.zeros((3, PAIRS, TERMS))
    places = [(half, first, second), (first, half, second), (first, second, half)]
    for face, place in enumerate(places):
        for column, values in enumerate(solid_values(*place)):
            degree = terms[column][1]
            expansion = project @ values @ project.T
            for spot, pair in enumerate(pair_list()):
                maps[face, spot, column] = scale * expansion[pair] / radius_scale**degree
    masks = np.zeros((3, 8, TERMS))
    for column, (kind, m, odd, _) in enumerate(power_list()):
        masks[0, (m + kind) % 2, column] = 1.0
        masks[1, kind, column] = 1.0
        masks[2, odd, column] = 1.0
    used = len(terms)
    maps[:, :, :used] = maps[:, :, :used] @ power_weights()
    folded = np.zeros((2, length // 2, length))
    parity = np.arange(length) % 2
    upper = 2.0 * sine[length // 2 :]
    folded[0] = upper * (parity == 0)
    folded[1] = upper * (parity == 1)
    return dict(
        sine=sine,
        eigen=eigen,
        cells=cells,
        legendre=legendre,
        columns=columns,
        spread=spread,
        own=own,
        edges=edges,
        maps=maps,
        masks=masks,
        folded=folded.reshape(length, length),
    )


def power_list():
    return [
        (kind, m, odd, power)
        for kind in range(2)
        for m in range(kind, COUNT)
        for odd in range(2)
        for power in range((ORDER - m - odd) // 2 + 1)
        if m + odd <= ORDER
    ]


def power_weights():
    poly = np.polynomial.polynomial
    columns = {term: spot for spot, term in enumerate(power_list())}
    harmonics, sector = {}, 1.0
    for m in range(COUNT):
        if m > 1:
            sector *= math.sqrt((2 * m - 1) / (2.0 * m))
        harmonics[m, m] = np.array([sector])
        for l in range(m + 1, COUNT):
            value = (2 * l - 1) * poly.polymul([0.0, 1.0], harmonics[l - 1, m])
            if l >= m + 2:
                value = poly.polysub(value, math.sqrt((l - 1) ** 2 - m * m) * harmonics[l - 2, m])
            harmonics[l, m] = value / math.sqrt(l * l - m * m)
    table = np.zeros((len(term_list()), len(columns)))
    for row, (kind, l, m) in enumerate(term_list()):
        odd = (l - m) % 2
        inner = harmonics[l, m][odd::2]
        shifted = np.zeros(1)
        for value in inner[::-1]:
            shifted = poly.polyadd(poly.polymul(shifted, [0.5, 0.5]), [value])
        factor = (1.0 if m == 0 else 2.0) / (4.0 * math.pi * radius_scale)
        for power in range(len(inner)):
            table[row, columns[kind, m, odd, power]] = (
                factor * shifted[power] / outer_ratio ** (l + 1)
            )
    return table


def evaluate(coef, unit_x, unit_y, unit_z):
    rows = {term: row for row, term in enumerate(power_list())}
    shifted = 2.0 * unit_z * unit_z - 1.0
    total = {}

    def weight(*term):
        row = rows[term]
        return jnp.broadcast_to(coef[row : row + 1, :], unit_z.shape)

    cosine, sine = None, None
    for m in range(COUNT):
        if m == 1:
            cosine, sine = unit_x, unit_y
        elif m > 1:
            cosine, sine = unit_x * cosine - unit_y * sine, unit_x * sine + unit_y * cosine
        for kind in range(1 if m == 0 else 2):
            for odd in range(2):
                if m + odd > ORDER:
                    continue
                top = (ORDER - m - odd) // 2
                value = weight(kind, m, odd, top)
                for power in range(top - 1, -1, -1):
                    value = value * shifted + weight(kind, m, odd, power)
                if m > 0:
                    value = value * (cosine, sine)[kind]
                key = (m % 2, kind, odd)
                total[key] = total[key] + value if key in total else value
    return {key: value * unit_z if key[2] else value for key, value in total.items()}


RESIDENT = pl.BlockSpec(memory_space=pltpu.VMEM)
SCALARS = pl.BlockSpec(memory_space=pltpu.SMEM)


def call(body, grid, in_specs, out_specs, out_shape, scratch, flops, aliases=None, limit=24):
    kernel = pl.pallas_call(
        body,
        grid=grid,
        in_specs=in_specs,
        out_specs=out_specs,
        out_shape=out_shape,
        scratch_shapes=scratch,
        input_output_aliases=aliases or {},
        cost_estimate=pl.CostEstimate(flops=flops, bytes_accessed=4 << 20, transcendentals=0),
        compiler_params=pltpu.CompilerParams(
            dimension_semantics=("arbitrary",) * len(grid), vmem_limit_bytes=limit << 20
        ),
    )

    def run(*args):
        placed = []
        for arg, spec in zip(args, in_specs):
            if spec is RESIDENT:
                arg = pltpu.with_memory_space_constraint(arg, pltpu.VMEM)
            elif spec.block_shape is not None:
                arg = pltpu.with_memory_space_constraint(arg, pltpu.HBM)
            placed.append(arg)
        return kernel(*placed)

    return run


def kept(*shape):
    return pltpu.VMEM(shape, F32)


def shards(charge_density):
    cells_a, cells_b, length = charge_density.shape
    groups_x, groups_y = lax.axis_size("gx"), lax.axis_size("gy")
    devices = groups_x * groups_y
    index_x, index_y = lax.axis_index("gx"), lax.axis_index("gy")
    tabs = constants(length)
    spacing = 1.0 / (length + 1)
    pack = max(1, 128 // cells_b)
    lanes = pack * cells_b
    wide = pack * length
    tiles = cells_a // pack
    depth = cells_b
    block = min(64, depth)
    blocks = depth // block
    modes = depth // groups_x
    ghosts = 2 * groups_x
    functions = COUNT + 2
    place = jnp.stack([index_x, index_y]).astype(jnp.int32)

    def const(name):
        return jnp.asarray(tabs[name].astype(np.float32))

    sine_high, sine_low = (jnp.asarray(t) for t in split_np(tabs["sine"]))
    sine_high = sine_high.reshape(groups_y, cells_b, length)
    sine_low = sine_low.reshape(groups_y, cells_b, length)
    parts_in = tiles // 4 if tiles % 4 == 0 else tiles
    uneven = parts_in < tiles
    going = [parts_in, 2 * parts_in, parts_in] if uneven else [tiles]
    coming = [parts_in, 2 * parts_in, parts_in] if uneven else [tiles]

    def starts_of(portions):
        return [sum(portions[:number]) for number in range(len(portions))]

    pair_limit = 24 if wide <= 512 else 44

    def fill_pairs(weights, high_ref, low_ref, index_y):
        weights[...] = jnp.zeros_like(weights)
        for shift in range(groups_y):
            peer = index_y ^ shift
            for item in range(pack):
                rows = pl.ds(shift * lanes + item * cells_b, cells_b)
                weights[0, rows, item * length : (item + 1) * length] = high_ref[peer]
                weights[1, rows, item * length : (item + 1) * length] = low_ref[peer]

    many = min(4, parts_in)

    def depth_body(place_ref, rho_ref, high_ref, low_ref, *rest):
        outs, table = rest[:groups_y], rest[groups_y]

        @pl.when(pl.program_id(0) == 0)
        def _():
            for shift in range(groups_y):
                peer = place_ref[1] ^ shift
                table[0, pl.ds(shift * cells_b, cells_b), :] = high_ref[peer]
                table[1, pl.ds(shift * cells_b, cells_b), :] = low_ref[peer]

        value = rho_ref[...].reshape(many * lanes, length)
        high, low = split(value)
        result = mul(table[0], high, NT) + mul(table[1], high, NT) + mul(table[0], low, NT)
        start = pl.program_id(0) * many
        for shift in range(groups_y):
            for item in range(many):
                outs[shift][start + item] = result[
                    shift * cells_b : (shift + 1) * cells_b, item * lanes : (item + 1) * lanes
                ]

    def pieces_of(count):
        return [kept(count, depth, lanes)] * groups_y

    table_spec = pl.BlockSpec((groups_y, cells_b, length), lambda t: (0, 0, 0))

    def depth_transform(number):
        steps, first = going[number] // many, starts_of(going)[number] // many
        return call(
            depth_body,
            (steps,),
            [
                SCALARS,
                pl.BlockSpec((many * pack, cells_b, length), lambda t: (t + first, 0, 0)),
                table_spec,
                table_spec,
            ],
            [RESIDENT] * groups_y,
            pieces_of(going[number]),
            [pltpu.VMEM((2, length, length), BF16)],
            10**9,
        )(
            place,
            charge_density,
            sine_high,
            sine_low,
        )

    def exchange(parts):
        received = [parts[0]]
        for shift in range(1, groups_y):
            ring = [(source, source ^ shift) for source in range(groups_y)]
            received.append(lax.ppermute(parts[shift], "gy", ring))
        return received

    received = []
    for number in range(len(going)):
        parts = depth_transform(number)
        received.append(exchange(parts))

    half = length // 2
    sine64 = tabs["sine"]
    scale = 2.0 / (length + 1)
    hat_all = scale * np.concatenate([tabs["legendre"] @ sine64, tabs["edges"]])
    hat_pad = -(-functions // 8) * 8
    hat_all = np.concatenate([hat_all, np.zeros((hat_pad - functions, length))])
    blank = np.zeros((1, length))
    lines = np.concatenate([blank, sine64, blank])
    spots = []
    for slab in range(groups_x):
        spots += [slab * cells_a, (slab + 1) * cells_a + 1]
    green_lines = lines[spots]
    chosen, green_row = [], {}
    for low in range(1, ghosts - 1):
        for high in range(low, ghosts - 1):
            green_row[low, high] = green_row[high, low] = len(chosen)
            chosen.append(scale * green_lines[low] * green_lines[high])
    chosen += [np.zeros(length)] * (-len(chosen) % 16)
    green = np.stack(chosen)
    eigen_column = np.broadcast_to(tabs["eigen"][:, None], (length, length))
    eigen_row = np.broadcast_to(tabs["eigen"][None, :], (8, length))
    cell_column = np.broadcast_to(tabs["cells"][:, None], (length, half))
    cell_row = np.broadcast_to(tabs["cells"][None, half:], (8, half))

    def put(table):
        return jnp.asarray(np.ascontiguousarray(table).astype(np.float32))

    def prepare_body(
        place_ref,
        column_ref,
        row_ref,
        line_ref,
        hat_ref,
        green_high_ref,
        green_low_ref,
        cell_column_ref,
        cell_row_ref,
        sine_high_ref,
        sine_low_ref,
        factor_ref,
        profile_ref,
        probe_ref,
        green_ref,
        unit_ref,
        pair_ref,
        table_ref,
        values,
        probe_high,
        probe_low,
    ):
        index_x, index_y = place_ref[0], place_ref[1]
        fill_pairs(pair_ref, sine_high_ref, sine_low_ref, index_y)
        for shift in range(groups_y):
            peer = index_y ^ shift
            table_ref[0, pl.ds(shift * cells_b, cells_b), :] = sine_high_ref[peer]
            table_ref[1, pl.ds(shift * cells_b, cells_b), :] = sine_low_ref[peer]
        own = pl.ds(pl.multiple_of(index_y * depth, depth), depth)
        values[...] = column_ref[own, :] + row_ref[0:1, :]
        value = values[...] + 2.0
        factor = inverted(value)
        running = factor
        factor_ref[0] = factor
        profile_ref[0] = running
        for row in range(1, cells_a):
            factor = inverted(value - factor)
            running = running * factor
            factor_ref[row] = factor
            profile_ref[row] = running
        for row in range(cells_a - 2, -1, -1):
            running = profile_ref[row] + factor_ref[row] * running
            profile_ref[row] = running
        for side in range(2):
            spot = index_x * cells_a + side * (cells_a + 1)
            table = line_ref[pl.ds(spot, 1), :] * hat_ref[...]
            high, low = split(table)
            probe_high[side * hat_pad : (side + 1) * hat_pad] = high
            probe_low[side * hat_pad : (side + 1) * hat_pad] = low

        def inverse_of(spot):
            return split(inverted(column_ref[...] + values[pl.ds(spot, 1), :]))

        def probe_step(number, carry):
            high, low = inverse_of(number)
            answer = (
                mul(probe_high[...], high, NN)
                + mul(probe_low[...], high, NN)
                + mul(probe_high[...], low, NN)
            )
            rows = pl.ds(pl.multiple_of(number * 2 * hat_pad, 8), 2 * hat_pad)
            for part in range(length // 128):
                probe_ref[part, rows, :] = answer[:, part * 128 : (part + 1) * 128]
            return carry

        lax.fori_loop(0, depth, probe_step, 0, unroll=4)

        def green_step(number, carry):
            high, low = inverse_of(index_x * modes + number)
            answer = (
                mul(green_high_ref[...], high, NN)
                + mul(green_low_ref[...], high, NN)
                + mul(green_high_ref[...], low, NN)
            )
            green_ref[pl.ds(number, 1)] = answer[None]
            return carry

        lax.fori_loop(0, modes, green_step, 0, unroll=min(2, modes))
        here = pl.ds(pl.multiple_of(index_x * cells_a, cells_a), cells_a)
        middle = jnp.full((8, half), 0.5, F32)[0:1]
        along = cell_row_ref[0:1, :]
        for begin, count, first, second, third in (
            (0, cells_a, cell_column_ref[here, :], middle, along),
            (cells_a, cells_a, cell_column_ref[here, :], along, middle),
            (2 * cells_a, half, middle, cell_column_ref[half:, :], along),
        ):
            inverse = 1.0 / jnp.sqrt(first * first + second * second + third * third)
            unit_ref[0, begin : begin + count] = first * inverse
            unit_ref[1, begin : begin + count] = second * inverse
            unit_ref[2, begin : begin + count] = third * inverse

    field = kept(cells_a, depth, length)
    green_high, green_low = (jnp.asarray(t) for t in split_np(green))
    inputs = (
        put(eigen_column),
        put(eigen_row),
        put(lines),
        put(hat_all),
        green_high,
        green_low,
        put(cell_column),
        put(cell_row),
        sine_high,
        sine_low,
    )

    def block_of(array):
        zeros = (0,) * array.ndim
        return pl.BlockSpec(array.shape, lambda k: zeros)

    tables = call(
        prepare_body,
        (1,),
        [SCALARS] + [block_of(array) for array in inputs],
        [RESIDENT] * 7,
        [
            field,
            field,
            kept(length // 128, depth * 2 * hat_pad, 128),
            kept(modes, green.shape[0], length),
            kept(3, 2 * cells_a + half, half),
            pltpu.VMEM((2, groups_y * lanes, wide), BF16),
            pltpu.VMEM((2, length, length), BF16),
        ],
        [
            pltpu.VMEM((depth, length), F32),
            pltpu.VMEM((2 * hat_pad, length), BF16),
            pltpu.VMEM((2 * hat_pad, length), BF16),
        ],
        10**10,
        limit=pair_limit,
    )(place, *inputs)
    legendre = put(tabs["legendre"])
    edge_rows = put(np.concatenate([tabs["edges"], np.zeros((6, length))]))
    edge_columns = put(np.broadcast_to(tabs["edges"][:, :, None], (2, length, 128)))
    column_high, column_low = (jnp.asarray(t) for t in split_np(tabs["columns"]))
    lookup = np.zeros((groups_y, 24, depth))
    lookup[:, : COUNT + 2] = (
        tabs["columns"][:, : COUNT + 2].T.reshape(COUNT + 2, groups_y, depth).transpose(1, 0, 2)
    )
    lookup = lookup.reshape(groups_y, 24, blocks, block).transpose(0, 2, 1, 3)
    lookup_high, lookup_low = (jnp.asarray(t) for t in split_np(lookup))
    spread = jnp.asarray(tabs["spread"].astype(np.float32)).astype(BF16)
    factors, profile, probe_table, green_table, units, pairs, table = tables

    def second_body(*refs):
        blocks_in = refs[:groups_y]
        weights, out_ref = refs[groups_y:]
        part_tiles = out_ref.shape[0] // pack
        for start in range(0, depth, block):
            value = jnp.concatenate(
                [
                    part[:, start : start + block, :].reshape(part_tiles * block, lanes)
                    for part in blocks_in
                ],
                axis=1,
            )
            result = triple(value, weights[0], weights[1], NN) * (spacing * spacing)
            for item in range(part_tiles):
                for inner in range(pack):
                    out_ref[item * pack + inner, start : start + block, :] = result[
                        item * block : (item + 1) * block, inner * length : (inner + 1) * length
                    ]

    sources = []
    for number, parts in enumerate(received):
        sources.append(
            call(
                second_body,
                (1,),
                [RESIDENT] * (groups_y + 1),
                RESIDENT,
                kept(going[number] * pack, depth, length),
                [],
                10**9,
                limit=pair_limit,
            )(*parts, pairs)
        )

    rows_now = min(32, block)

    def solve_body(place_ref, leg_ref, *refs):
        given = refs[: len(going)]
        (
            factor_ref,
            probe_ref,
            column_high_ref,
            column_low_ref,
            lookup_high_ref,
            lookup_low_ref,
            spread_ref,
            own_ref,
            map_ref,
            mask_ref,
            field_ref,
            moment_ref,
            energy_ref,
            tensor,
        ) = refs[len(going) :]
        index_x, index_y = place_ref[0], place_ref[1]
        begin = jnp.where(index_x == 0, 1.0, 0.0)
        finish = jnp.where(index_x == groups_x - 1, 1.0, 0.0)
        step = pl.program_id(0)
        base = pl.multiple_of(step * block, block)
        window = pl.ds(base, block)

        @pl.when(step == 0)
        def _():
            tensor[...] = jnp.zeros_like(tensor)
            energy_ref[...] = jnp.zeros_like(energy_ref)

        def source(row, begin_row):
            starts = starts_of(going)
            number = max(n for n in range(len(going)) if starts[n] * pack <= row)
            return given[number][row - starts[number] * pack, pl.ds(begin_row, rows_now), :]

        def eliminate(begin_row):
            strip = pl.ds(begin_row, rows_now)
            running = source(0, begin_row) * factor_ref[0, strip, :]
            field_ref[0, strip, :] = running
            for row in range(1, cells_a):
                running = (source(row, begin_row) + running) * factor_ref[row, strip, :]
                field_ref[row, strip, :] = running
            energy = source(cells_a - 1, begin_row) * running
            for row in range(cells_a - 2, -1, -1):
                running = field_ref[row, strip, :] + factor_ref[row, strip, :] * running
                field_ref[row, strip, :] = running
                energy = energy + source(row, begin_row) * running
            energy = jnp.sum(energy.reshape(rows_now // 8, 8, length), axis=0)
            for part in range(length // 128):
                energy_ref[...] += energy[:, part * 128 : (part + 1) * 128]

        for offset in range(0, block, rows_now):
            eliminate(pl.multiple_of(base + offset, rows_now))
        first, last = field_ref[0, window, :], field_ref[cells_a - 1, window, :]
        table_high, table_low = column_high_ref[...], column_low_ref[...]
        rows_high = lookup_high_ref[index_y, step]
        rows_low = lookup_low_ref[index_y, step]

        def contract(stack, count):
            answer = triple(stack, table_high, table_low, NN)
            upper, lower = split(answer)
            outs = []
            for item in range(count):
                high = upper[item * block : (item + 1) * block]
                low = lower[item * block : (item + 1) * block]
                outs.append(
                    mul(rows_high, high, NN) + mul(rows_low, high, NN) + mul(rows_high, low, NN)
                )
            return outs

        many_rows = min(16, cells_a)
        for start in range(0, cells_a, many_rows):
            stack = field_ref[start : start + many_rows, window, :].reshape(
                many_rows * block, length
            )
            outs = contract(stack, many_rows)
            for item in range(COUNT):
                value = tensor[item]
                for inner, out in enumerate(outs):
                    value = value + leg_ref[item, index_x * cells_a + start + inner] * out
                tensor[item] = value
            if start == 0:
                tensor[COUNT] += begin * outs[0]
                tensor[COUNT + 1] -= begin * outs[0]
            if start + many_rows == cells_a:
                tensor[COUNT] += finish * outs[-1]
                tensor[COUNT + 1] += finish * outs[-1]

        def probe_row(item):
            rows = pl.ds(base * 2 * hat_pad + item, block, stride=2 * hat_pad)
            return jnp.concatenate(
                [probe_ref[part, rows, :] for part in range(length // 128)], axis=1
            )

        group = 10
        for start in range(0, functions, group):
            items = range(start, min(start + group, functions))
            stack = jnp.concatenate(
                [
                    probe_row(item) * first + probe_row(hat_pad + item) * last
                    for item in items
                ],
                axis=0,
            )
            for item, out in zip(items, contract(stack, len(items))):
                tensor[item] += out

        @pl.when(step == blocks - 1)
        def _():
            rows = lax.broadcasted_iota(jnp.int32, (8, PAIRS), 0)

            def flatten(matrix, kind):
                high, low = split(matrix)
                answer = mul(high, spread_ref[kind], NN) + mul(low, spread_ref[kind], NN)
                return jnp.sum(answer * own_ref[1 - kind], axis=0, keepdims=True)

            moments = jnp.zeros((8, TERMS), F32)
            for face in range(3):
                stack = jnp.zeros((8, PAIRS), F32)
                for parity in range(2):
                    if face == 0:
                        value = flatten(tensor[COUNT + parity], 0)
                    elif face == 1:
                        value = jnp.zeros((1, PAIRS), F32)
                        for item in range(COUNT):
                            column = tensor[item, :, COUNT + parity : COUNT + parity + 1]
                            chosen = own_ref[0, item : item + 1, :] * own_ref[1]
                            value = value + jnp.sum(column * chosen, axis=0, keepdims=True)
                    else:
                        matrix = jnp.concatenate(
                            [
                                tensor[item, COUNT + parity : COUNT + parity + 1, :]
                                for item in range(COUNT)
                            ]
                            + [jnp.zeros((24 - COUNT, 128), F32)],
                            axis=0,
                        )
                        high, low = split(matrix)
                        answer = mul(high, spread_ref[1], NN) + mul(low, spread_ref[1], NN)
                        value = jnp.sum(answer * own_ref[0], axis=0, keepdims=True)
                    stack = jnp.where(rows == parity, value, stack)
                moments = moments + exact(stack, map_ref[face], NN) * mask_ref[face]
            moments = jnp.sum(moments, axis=0, keepdims=True)
            moment_ref[...] = jnp.broadcast_to(moments[None], moment_ref.shape)

    solved, moments, energy_one = call(
        solve_body,
        (blocks,),
        [SCALARS] * 2 + [RESIDENT] * (len(going) + 10),
        [RESIDENT] * 3,
        [field, kept(devices, 1, TERMS), kept(8, 128)],
        [
            pltpu.VMEM((24, 24, 128), F32),
        ],
        10**9,
    )(
        place,
        legendre,
        *sources,
        factors,
        probe_table,
        column_high,
        column_low,
        lookup_high,
        lookup_low,
        spread,
        const("own"),
        const("maps"),
        const("masks"),
    )
    shared = lax.all_to_all(moments, ("gx", "gy"), 0, 0, tiled=True)

    folded_high, folded_low = (jnp.asarray(t) for t in split_np(tabs["folded"]))
    local_high, local_low = (
        jnp.asarray(np.ascontiguousarray(t.T).reshape(groups_y, depth, length))
        for t in split_np(tabs["folded"])
    )
    strip = min(32, cells_a)
    shares_count = block // modes
    face_rows = min(FACE_ROWS, block)

    def source_body(
        place_ref,
        share_ref,
        unit_ref,
        folded_high_ref,
        folded_low_ref,
        local_high_ref,
        local_low_ref,
        row_ref,
        column_ref,
        factor_ref,
        solved_ref,
        total_ref,
        near_ref,
        energy_ref,
        coef,
        values,
        plane_x,
        plane_y,
        plane_z,
        lines_y,
        lines_z,
        walls,
    ):
        index_x, index_y = place_ref[0], place_ref[1]
        begin = jnp.where(index_x == 0, 1.0, 0.0)
        finish = jnp.where(index_x == groups_x - 1, 1.0, 0.0)

        step = pl.program_id(0)
        window = pl.ds(pl.multiple_of(step * block, block), block)

        @pl.when(step == 0)
        def _():
            ones = jnp.full((8, 128), 0.125, F32)
            shares = jnp.broadcast_to(jnp.sum(share_ref[...], axis=0), (8, TERMS))
            coef[...] = exact(shares, ones, TN)
            energy_ref[...] = jnp.zeros_like(energy_ref)

            def one_strip(number, carry):
                window = pl.ds(pl.multiple_of(number * strip, strip), strip)
                classes = evaluate(
                    coef, unit_ref[0, window, :], unit_ref[1, window, :], unit_ref[2, window, :]
                )
                for (azimuth, kind, odd), value in classes.items():
                    values[azimuth * 4 + kind * 2 + odd, window, :] = value
                return carry

            lax.fori_loop(0, (2 * cells_a + half) // strip, one_strip, 0)
            for kind in range(2):
                for odd in range(2):
                    for start, target, row, column in (
                        (0, plane_y, kind, odd),
                        (cells_a, plane_z, odd, kind),
                    ):
                        target[
                            row * cells_a : (row + 1) * cells_a, column * half : (column + 1) * half
                        ] = (
                            values[kind * 2 + odd, start : start + cells_a, :]
                            + values[4 + kind * 2 + odd, start : start + cells_a, :]
                        )
                    even, other = (
                        values[parity * 4 + kind * 2 + odd, 2 * cells_a :, :]
                        for parity in (kind, 1 - kind)
                    )
                    plane_x[
                        kind * half : (kind + 1) * half, odd * half : (odd + 1) * half
                    ] = even + (finish - begin) * other
            folded_tables = folded_high_ref[...], folded_low_ref[...]
            local_tables = local_high_ref[index_y], local_low_ref[index_y]

            def across(plane):
                upper, lower = split(plane)
                high, low = local_tables
                return mul(high, upper, NT) + mul(low, upper, NT) + mul(high, lower, NT)

            lines_z[...] = triple(plane_z[...], *folded_tables, NN)
            lines_y[...] = across(plane_y[...])
            wall = triple(across(plane_x[...]), *folded_tables, NN)
            walls[0] = begin * wall
            walls[1] = finish * wall


        def eliminate(offset):
            begin_row = pl.multiple_of(step * block + offset, face_rows)
            window = pl.ds(begin_row, face_rows)
            here = pl.ds(pl.multiple_of(index_y * depth + begin_row, face_rows), face_rows)
            columns = [
                jnp.concatenate([column_ref[parity, here, :]] * (length // 128), axis=1)
                for parity in range(2)
            ]
            line_block = lines_y[window, :]
            energy = jnp.zeros((face_rows, length), F32)
            running = None
            for row in range(cells_a):
                value = None
                for parity in range(2):
                    spot = parity * cells_a + row
                    term = line_block[:, spot : spot + 1] * row_ref[parity : parity + 1, :]
                    value = term if value is None else value + term
                    value = value + lines_z[spot : spot + 1, :] * columns[parity]
                if row == 0:
                    value = value + walls[0, window, :]
                if row == cells_a - 1:
                    value = value + walls[1, window, :]
                energy = energy + value * solved_ref[row, window, :]
                running = value if running is None else value + running
                running = running * factor_ref[row, window, :]
                total_ref[row, window, :] = running
            nears = [solved_ref[0, window, :], solved_ref[cells_a - 1, window, :], None, running]
            total_ref[cells_a - 1, window, :] = nears[1] + running
            for row in range(cells_a - 2, -1, -1):
                running = total_ref[row, window, :] + factor_ref[row, window, :] * running
                total_ref[row, window, :] = solved_ref[row, window, :] + running
            nears[2] = running
            for item in range(face_rows // modes):
                for number, value in enumerate(nears):
                    near_ref[(step * block + offset) // modes + item, number] = value[
                        item * modes : (item + 1) * modes
                    ]
            energy = jnp.sum(energy.reshape(face_rows // 8, 8, length), axis=0)
            for part in range(length // 128):
                energy_ref[...] += energy[:, part * 128 : (part + 1) * 128]

        for offset in range(0, block, face_rows):
            eliminate(offset)

    total, nears, energy_two = call(
        source_body,
        (blocks,),
        [SCALARS] + [RESIDENT] * 10,
        [RESIDENT] * 3,
        [field, kept(groups_x, 4, modes, length), kept(8, 128)],
        [
            pltpu.VMEM((TERMS, 128), F32),
            kept(8, 2 * cells_a + half, half),
            pltpu.VMEM((length, length), F32),
            pltpu.VMEM((2 * cells_a, length), F32),
            pltpu.VMEM((2 * cells_a, length), F32),
            pltpu.VMEM((depth, 2 * cells_a), F32),
            pltpu.VMEM((2 * cells_a, length), F32),
            pltpu.VMEM((2, depth, length), F32),
        ],
        10**9,
    )(
        place,
        shared,
        units,
        folded_high,
        folded_low,
        local_high,
        local_low,
        edge_rows,
        edge_columns,
        factors,
        solved,
    )

    gathered = lax.all_to_all(nears, "gx", 0, 0, tiled=True)

    def ghost_body(near_ref, green_ref, one_ref, two_ref, out_ref):
        first = [near_ref[s, 0] for s in range(groups_x)]
        last = [near_ref[s, 1] for s in range(groups_x)]
        other_first = [near_ref[s, 2] for s in range(groups_x)]
        other_last = [near_ref[s, 3] for s in range(groups_x)]
        energy_one = jnp.zeros((modes, length), F32)
        energy_two = jnp.zeros((modes, length), F32)
        for slab in range(groups_x):
            for side in range(2):
                value = jnp.zeros((modes, length), F32)
                other = jnp.zeros((modes, length), F32)
                neighbour = slab + (1 if side else -1)
                if 0 <= neighbour < groups_x:
                    value = (first if side else last)[neighbour]
                    other = (other_first if side else other_last)[neighbour]
                    for s in range(groups_x):
                        for end, one, two in (
                            (0, first, other_first),
                            (1, last, other_last),
                        ):
                            row = green_row.get((2 * slab + side, 2 * s + end))
                            if row is not None:
                                green = green_ref[:, row, :]
                                value = value + green * one[s]
                                other = other + green * two[s]
                energy_one = energy_one + value * (last if side else first)[slab]
                energy_two = energy_two + value * (other_last if side else other_first)[slab]
                out_ref[slab, side * modes : (side + 1) * modes, :] = value + other
        top = lax.broadcasted_iota(jnp.int32, (8, 128), 0) == 0
        for number, (local_ref, value) in enumerate(((one_ref, energy_one), (two_ref, energy_two))):
            value = jnp.sum(value, axis=0, keepdims=True)
            line = value[:, 0:128]
            for part in range(1, length // 128):
                line = line + value[:, part * 128 : (part + 1) * 128]
            tile = local_ref[...] + jnp.where(top, line, 0.0)
            for slab in range(groups_x):
                out_ref[slab, 2 * modes : 2 * modes + 8, number * 128 : (number + 1) * 128] = tile

    height = 2 * modes + 8
    answers = call(
        ghost_body, (1,), [RESIDENT] * 4, RESIDENT, kept(groups_x, height, length), [], 10**8
    )(gathered, green_table, energy_one, energy_two)
    returned = lax.all_to_all(answers, "gx", 0, 0, tiled=True)

    def back_body(number, total_ref, profile_ref, ghost_ref, weights, *rest):
        outs, energy_ref = rest[:groups_y], rest[groups_y]
        energy_ref[...] = jnp.sum(ghost_ref[:, 2 * modes : 2 * modes + 8, 0:256], axis=0)
        for step in range(blocks):
            back_block(total_ref, profile_ref, ghost_ref, outs, weights, step, number)

    def back_block(total_ref, profile_ref, ghost_ref, outs, weights, step, number):
        window = pl.ds(step * block, block)
        ghosts_here = [
            jnp.concatenate(
                [
                    ghost_ref[step * shares_count + item, side * modes : (side + 1) * modes, :]
                    for item in range(shares_count)
                ],
                axis=0,
            )
            for side in range(2)
        ]

        parts = []
        for item in range(starts_of(coming)[number], starts_of(coming)[number] + coming[number]):
            inner = []
            for row in range(item * pack, (item + 1) * pack):
                inner.append(
                    total_ref[row, window, :]
                    + profile_ref[row, window, :] * ghosts_here[0]
                    + profile_ref[cells_a - 1 - row, window, :] * ghosts_here[1]
                )
            parts.append(jnp.concatenate(inner, axis=1))
        result = triple(jnp.concatenate(parts, axis=0), weights[0], weights[1], NT)
        for shift in range(groups_y):
            for item in range(coming[number]):
                outs[shift][item, window, :] = result[
                    item * block : (item + 1) * block, shift * lanes : (shift + 1) * lanes
                ]

    arrived = []
    for number in range(len(coming)):
        *parts, tile_now = call(
            functools.partial(back_body, number),
            (1,),
            [RESIDENT] * 4,
            [RESIDENT] * (groups_y + 1),
            pieces_of(coming[number]) + [kept(8, 256)],
            [],
            10**9,
            limit=pair_limit,
        )(total, profile, returned, pairs)
        energy_tile = tile_now if number == 0 else energy_tile
        arrived.append(exchange(parts))
    energy_tiles = exchange([energy_tile] * groups_y)

    norm = (2.0 / (length + 1)) ** 2

    def last_body(*refs):
        blocks_in = refs[:groups_y]
        table, out_ref = refs[groups_y], refs[-1]
        start = pl.program_id(0) * many
        values = [
            jnp.concatenate([part[start + item] for part in blocks_in], axis=0).T
            for item in range(many)
        ]
        result = triple(jnp.concatenate(values, axis=0), table[0], table[1], NN) * norm
        out_ref[...] = result.reshape(many * pack, cells_b, length)

    def final_body(*refs):
        tiles_in = refs[-2 - groups_y : -2]
        energy_ref = refs[-1]
        last_body(*refs[: groups_y + 1], refs[-2])

        @pl.when(pl.program_id(0) == 0)
        def _():
            value = tiles_in[0][...]
            for tile in tiles_in[1:]:
                value = value + tile[...]
            factor = spacing * norm
            first = jnp.sum(value[:, 0:128]) * factor
            energy_ref[0] = first
            energy_ref[1] = first + jnp.sum(value[:, 128:256]) * factor

    shape = jax.ShapeDtypeStruct(charge_density.shape, F32)
    base_specs = [RESIDENT] * (groups_y + 1)
    out_block = (many * pack, cells_b, length)
    potential = None
    for number in range(len(coming)):
        steps, first = coming[number] // many, starts_of(coming)[number] // many
        inputs = [*arrived[number], table]
        specs, aliases = list(base_specs), None
        if number > 0:
            aliases = {len(inputs): 0}
            inputs.append(potential)
            specs.append(pl.BlockSpec(memory_space=pl.ANY))
        out_spec = pl.BlockSpec(out_block, lambda t, first=first: (t + first, 0, 0))
        if number < len(coming) - 1:
            potential = call(
                last_body, (steps,), specs, out_spec, shape, [], 10**9, aliases
            )(*inputs)
        else:
            potential, energies = call(
                final_body,
                (steps,),
                specs + [RESIDENT] * groups_y,
                [out_spec, SCALARS],
                [shape, jax.ShapeDtypeStruct((2,), F32)],
                [],
                10**9,
                aliases,
            )(*inputs, *energy_tiles)
    return potential, energies


def solution(mesh):
    placed = (P("gx", "gy", None),)
    return jax.shard_map(
        shards, mesh=mesh, in_specs=placed, out_specs=(P("gx", "gy", None), P()), check_vma=False
    )
```

```python
import functools
import math

import jax
import jax.numpy as jnp
import numpy as np
from jax import lax
from jax.experimental import pallas as pl
from jax.experimental.pallas import tpu as pltpu
from jax.sharding import PartitionSpec as P

ORDER = 16
COUNT = ORDER + 1
PAIRS = 256
NEWTON = 1
FACE_ROWS = 8
TERMS = 384
outer_ratio = 1.1
radius_scale = math.sqrt(3.0) / 2.0
F32 = jnp.float32
BF16 = jnp.bfloat16
EXACT = lax.Precision.HIGHEST


NN = (((1,), (0,)), ((), ()))
NT = (((1,), (1,)), ((), ()))
TN = (((0,), (0,)), ((), ()))


def pair_list():
    return [(p, q) for p in range(COUNT) for q in range(COUNT - p)]


def term_list():
    terms = [(0, l, m) for m in range(COUNT) for l in range(m, COUNT)]
    terms += [(1, l, m) for m in range(1, COUNT) for l in range(m, COUNT)]
    return terms


def split_np(table):
    import ml_dtypes

    high = table.astype(np.float32).astype(ml_dtypes.bfloat16)
    low = (table - high.astype(np.float64)).astype(np.float32).astype(ml_dtypes.bfloat16)
    return high, low


def split(value):
    high = value.astype(BF16)
    return high, (value - high.astype(F32)).astype(BF16)


def mul(left, right, dims):
    return lax.dot_general(left, right, dims, preferred_element_type=F32)


def triple(left, high, low, dims):
    first, second = split(left)
    return mul(first, high, dims) + mul(first, low, dims) + mul(second, high, dims)


def inverted(value):
    guess = pl.reciprocal(value, approx=True)
    for _ in range(NEWTON):
        guess = guess * (2.0 - value * guess)
    return guess


def exact(left, right, dims):
    return lax.dot_general(left, right, dims, precision=EXACT, preferred_element_type=F32)


def solid_values(x, y, z):
    squared = x * x + y * y + z * z
    cosine, sine = {}, {}
    cosine[0, 0], sine[0, 0] = np.ones_like(x), np.zeros_like(x)
    for l in range(1, COUNT):
        scale = math.sqrt((2 * l - 1) / (2.0 * l)) if l > 1 else 1.0
        cosine[l, l] = scale * (x * cosine[l - 1, l - 1] - y * sine[l - 1, l - 1])
        sine[l, l] = scale * (x * sine[l - 1, l - 1] + y * cosine[l - 1, l - 1])
    for table in (cosine, sine):
        for m in range(COUNT):
            for l in range(m + 1, COUNT):
                older = table[l - 2, m] if l - 2 >= m else np.zeros_like(x)
                table[l, m] = (
                    (2 * l - 1) * z * table[l - 1, m]
                    - math.sqrt((l - 1) ** 2 - m * m) * squared * older
                ) / math.sqrt(l * l - m * m)
    return [(cosine, sine)[kind][l, m] for kind, l, m in term_list()]


@functools.cache
def constants(length):
    step = length + 1
    index = np.arange(length) + 1
    sine = np.sin(np.pi * ((index[:, None] * index[None, :]) % (2 * step)) / step)
    eigen = 4.0 * np.sin(np.pi * index / (2.0 * step)) ** 2
    cells = (np.arange(length) - (length - 1) / 2.0) / step
    legendre = np.stack(
        [np.polynomial.legendre.legval(2 * cells, np.eye(COUNT)[p]) for p in range(COUNT)]
    )
    hat = legendre @ sine
    edges = np.stack([sine[0] + sine[-1], sine[-1] - sine[0]])
    lookup = np.concatenate([hat, edges])
    columns = np.zeros((length, 128))
    columns[:, : COUNT + 2] = lookup.T
    spread = np.zeros((2, 128, PAIRS))
    own = np.zeros((2, 24, PAIRS))
    for spot, pair in enumerate(pair_list()):
        for kind in range(2):
            spread[kind, pair[kind], spot] = 1.0
            own[kind, pair[kind], spot] = 1.0
    nodes, weights = np.polynomial.legendre.leggauss(COUNT + 3)
    basis = np.stack([np.polynomial.legendre.legval(nodes, np.eye(COUNT)[p]) for p in range(COUNT)])
    project = basis * weights[None, :] * (2 * np.arange(COUNT)[:, None] + 1) / 2.0
    first, second = np.meshgrid(nodes / 2.0, nodes / 2.0, indexing="ij")
    half = np.full_like(first, 0.5)
    terms = term_list()
    scale = (1.0 / step) * (2.0 / step) ** 2
    maps = np.zeros((3, PAIRS, TERMS))
    places = [(half, first, second), (first, half, second), (first, second, half)]
    for face, place in enumerate(places):
        for column, values in enumerate(solid_values(*place)):
            degree = terms[column][1]
            expansion = project @ values @ project.T
            for spot, pair in enumerate(pair_list()):
                maps[face, spot, column] = scale * expansion[pair] / radius_scale**degree
    masks = np.zeros((3, 8, TERMS))
    for column, (kind, m, odd, _) in enumerate(power_list()):
        masks[0, (m + kind) % 2, column] = 1.0
        masks[1, kind, column] = 1.0
        masks[2, odd, column] = 1.0
    used = len(terms)
    maps[:, :, :used] = maps[:, :, :used] @ power_weights()
    folded = np.zeros((2, length // 2, length))
    parity = np.arange(length) % 2
    upper = 2.0 * sine[length // 2 :]
    folded[0] = upper * (parity == 0)
    folded[1] = upper * (parity == 1)
    return dict(
        sine=sine,
        eigen=eigen,
        cells=cells,
        legendre=legendre,
        columns=columns,
        spread=spread,
        own=own,
        edges=edges,
        maps=maps,
        masks=masks,
        folded=folded.reshape(length, length),
    )


def power_list():
    return [
        (kind, m, odd, power)
        for kind in range(2)
        for m in range(kind, COUNT)
        for odd in range(2)
        for power in range((ORDER - m - odd) // 2 + 1)
        if m + odd <= ORDER
    ]


def power_weights():
    poly = np.polynomial.polynomial
    columns = {term: spot for spot, term in enumerate(power_list())}
    harmonics, sector = {}, 1.0
    for m in range(COUNT):
        if m > 1:
            sector *= math.sqrt((2 * m - 1) / (2.0 * m))
        harmonics[m, m] = np.array([sector])
        for l in range(m + 1, COUNT):
            value = (2 * l - 1) * poly.polymul([0.0, 1.0], harmonics[l - 1, m])
            if l >= m + 2:
                value = poly.polysub(value, math.sqrt((l - 1) ** 2 - m * m) * harmonics[l - 2, m])
            harmonics[l, m] = value / math.sqrt(l * l - m * m)
    table = np.zeros((len(term_list()), len(columns)))
    for row, (kind, l, m) in enumerate(term_list()):
        odd = (l - m) % 2
        inner = harmonics[l, m][odd::2]
        shifted = np.zeros(1)
        for value in inner[::-1]:
            shifted = poly.polyadd(poly.polymul(shifted, [0.5, 0.5]), [value])
        factor = (1.0 if m == 0 else 2.0) / (4.0 * math.pi * radius_scale)
        for power in range(len(inner)):
            table[row, columns[kind, m, odd, power]] = (
                factor * shifted[power] / outer_ratio ** (l + 1)
            )
    return table


def evaluate(coef, unit_x, unit_y, unit_z):
    rows = {term: row for row, term in enumerate(power_list())}
    shifted = 2.0 * unit_z * unit_z - 1.0
    total = {}

    def weight(*term):
        row = rows[term]
        return jnp.broadcast_to(coef[row : row + 1, :], unit_z.shape)

    cosine, sine = None, None
    for m in range(COUNT):
        if m == 1:
            cosine, sine = unit_x, unit_y
        elif m > 1:
            cosine, sine = unit_x * cosine - unit_y * sine, unit_x * sine + unit_y * cosine
        for kind in range(1 if m == 0 else 2):
            for odd in range(2):
                if m + odd > ORDER:
                    continue
                top = (ORDER - m - odd) // 2
                value = weight(kind, m, odd, top)
                for power in range(top - 1, -1, -1):
                    value = value * shifted + weight(kind, m, odd, power)
                if m > 0:
                    value = value * (cosine, sine)[kind]
                key = (m % 2, kind, odd)
                total[key] = total[key] + value if key in total else value
    return {key: value * unit_z if key[2] else value for key, value in total.items()}


RESIDENT = pl.BlockSpec(memory_space=pltpu.VMEM)
SCALARS = pl.BlockSpec(memory_space=pltpu.SMEM)


def call(body, grid, in_specs, out_specs, out_shape, scratch, flops, aliases=None, limit=24):
    kernel = pl.pallas_call(
        body,
        grid=grid,
        in_specs=in_specs,
        out_specs=out_specs,
        out_shape=out_shape,
        scratch_shapes=scratch,
        input_output_aliases=aliases or {},
        cost_estimate=pl.CostEstimate(flops=flops, bytes_accessed=4 << 20, transcendentals=0),
        compiler_params=pltpu.CompilerParams(
            dimension_semantics=("arbitrary",) * len(grid), vmem_limit_bytes=limit << 20
        ),
    )

    def run(*args):
        placed = []
        for arg, spec in zip(args, in_specs):
            if spec is RESIDENT:
                arg = pltpu.with_memory_space_constraint(arg, pltpu.VMEM)
            elif spec.block_shape is not None:
                arg = pltpu.with_memory_space_constraint(arg, pltpu.HBM)
            placed.append(arg)
        return kernel(*placed)

    return run


def kept(*shape):
    return pltpu.VMEM(shape, F32)


def shards(charge_density):
    cells_a, cells_b, length = charge_density.shape
    groups_x, groups_y = lax.axis_size("gx"), lax.axis_size("gy")
    devices = groups_x * groups_y
    index_x, index_y = lax.axis_index("gx"), lax.axis_index("gy")
    tabs = constants(length)
    spacing = 1.0 / (length + 1)
    pack = max(1, 128 // cells_b)
    lanes = pack * cells_b
    wide = pack * length
    tiles = cells_a // pack
    depth = cells_b
    block = min(64, depth)
    blocks = depth // block
    modes = depth // groups_x
    ghosts = 2 * groups_x
    functions = COUNT + 2
    place = jnp.stack([index_x, index_y]).astype(jnp.int32)

    def const(name):
        return jnp.asarray(tabs[name].astype(np.float32))

    sine_high, sine_low = (jnp.asarray(t) for t in split_np(tabs["sine"]))
    sine_high = sine_high.reshape(groups_y, cells_b, length)
    sine_low = sine_low.reshape(groups_y, cells_b, length)
    parts_in = tiles // 4 if tiles % 4 == 0 else tiles
    uneven = parts_in < tiles
    going = [parts_in, 2 * parts_in, parts_in] if uneven else [tiles]
    coming = [parts_in, 2 * parts_in, parts_in] if uneven else [tiles]

    def starts_of(portions):
        return [sum(portions[:number]) for number in range(len(portions))]

    pair_limit = 24 if wide <= 512 else 44

    def fill_pairs(weights, high_ref, low_ref, index_y):
        weights[...] = jnp.zeros_like(weights)
        for shift in range(groups_y):
            peer = index_y ^ shift
            for item in range(pack):
                rows = pl.ds(shift * lanes + item * cells_b, cells_b)
                weights[0, rows, item * length : (item + 1) * length] = high_ref[peer]
                weights[1, rows, item * length : (item + 1) * length] = low_ref[peer]

    many = min(4, parts_in)

    def depth_body(place_ref, rho_ref, high_ref, low_ref, *rest):
        outs, table = rest[:groups_y], rest[groups_y]

        @pl.when(pl.program_id(0) == 0)
        def _():
            for shift in range(groups_y):
                peer = place_ref[1] ^ shift
                table[0, pl.ds(shift * cells_b, cells_b), :] = high_ref[peer]
                table[1, pl.ds(shift * cells_b, cells_b), :] = low_ref[peer]

        value = rho_ref[...].reshape(many * lanes, length)
        high, low = split(value)
        result = mul(table[0], high, NT) + mul(table[1], high, NT) + mul(table[0], low, NT)
        start = pl.program_id(0) * many
        for shift in range(groups_y):
            for item in range(many):
                outs[shift][start + item] = result[
                    shift * cells_b : (shift + 1) * cells_b, item * lanes : (item + 1) * lanes
                ]

    def pieces_of(count):
        return [kept(count, depth, lanes)] * groups_y

    table_spec = pl.BlockSpec((groups_y, cells_b, length), lambda t: (0, 0, 0))

    def depth_transform(number):
        steps, first = going[number] // many, starts_of(going)[number] // many
        return call(
            depth_body,
            (steps,),
            [
                SCALARS,
                pl.BlockSpec((many * pack, cells_b, length), lambda t: (t + first, 0, 0)),
                table_spec,
                table_spec,
            ],
            [RESIDENT] * groups_y,
            pieces_of(going[number]),
            [pltpu.VMEM((2, length, length), BF16)],
            10**9,
        )(
            place,
            charge_density,
            sine_high,
            sine_low,
        )

    def exchange(parts):
        received = [parts[0]]
        for shift in range(1, groups_y):
            ring = [(source, source ^ shift) for source in range(groups_y)]
            received.append(lax.ppermute(parts[shift], "gy", ring))
        return received

    received = []
    for number in range(len(going)):
        parts = depth_transform(number)
        received.append(exchange(parts))

    half = length // 2
    sine64 = tabs["sine"]
    scale = 2.0 / (length + 1)
    hat_all = scale * np.concatenate([tabs["legendre"] @ sine64, tabs["edges"]])
    hat_pad = -(-functions // 8) * 8
    hat_all = np.concatenate([hat_all, np.zeros((hat_pad - functions, length))])
    blank = np.zeros((1, length))
    lines = np.concatenate([blank, sine64, blank])
    spots = []
    for slab in range(groups_x):
        spots += [slab * cells_a, (slab + 1) * cells_a + 1]
    green_lines = lines[spots]
    chosen, green_row = [], {}
    for low in range(1, ghosts - 1):
        for high in range(low, ghosts - 1):
            green_row[low, high] = green_row[high, low] = len(chosen)
            chosen.append(scale * green_lines[low] * green_lines[high])
    chosen += [np.zeros(length)] * (-len(chosen) % 16)
    green = np.stack(chosen)
    eigen_column = np.broadcast_to(tabs["eigen"][:, None], (length, length))
    eigen_row = np.broadcast_to(tabs["eigen"][None, :], (8, length))
    cell_column = np.broadcast_to(tabs["cells"][:, None], (length, half))
    cell_row = np.broadcast_to(tabs["cells"][None, half:], (8, half))

    def put(table):
        return jnp.asarray(np.ascontiguousarray(table).astype(np.float32))

    def prepare_body(
        place_ref,
        column_ref,
        row_ref,
        line_ref,
        hat_ref,
        green_high_ref,
        green_low_ref,
        cell_column_ref,
        cell_row_ref,
        sine_high_ref,
        sine_low_ref,
        factor_ref,
        profile_ref,
        probe_ref,
        green_ref,
        unit_ref,
        pair_ref,
        table_ref,
        legendre_ref,
        values,
        probe_high,
        probe_low,
    ):
        index_x, index_y = place_ref[0], place_ref[1]
        fill_pairs(pair_ref, sine_high_ref, sine_low_ref, index_y)
        for shift in range(groups_y):
            peer = index_y ^ shift
            table_ref[0, pl.ds(shift * cells_b, cells_b), :] = sine_high_ref[peer]
            table_ref[1, pl.ds(shift * cells_b, cells_b), :] = sine_low_ref[peer]
        own = pl.ds(pl.multiple_of(index_y * depth, depth), depth)
        values[...] = column_ref[own, :] + row_ref[0:1, :]
        value = values[...] + 2.0
        factor = inverted(value)
        running = factor
        factor_ref[0] = factor
        profile_ref[0] = running
        for row in range(1, cells_a):
            factor = inverted(value - factor)
            running = running * factor
            factor_ref[row] = factor
            profile_ref[row] = running
        for row in range(cells_a - 2, -1, -1):
            running = profile_ref[row] + factor_ref[row] * running
            profile_ref[row] = running
        for side in range(2):
            spot = index_x * cells_a + side * (cells_a + 1)
            table = line_ref[pl.ds(spot, 1), :] * hat_ref[...]
            high, low = split(table)
            probe_high[side * hat_pad : (side + 1) * hat_pad] = high
            probe_low[side * hat_pad : (side + 1) * hat_pad] = low

        def inverse_of(spot):
            return split(inverted(column_ref[...] + values[pl.ds(spot, 1), :]))

        def probe_step(number, carry):
            high, low = inverse_of(number)
            answer = (
                mul(probe_high[...], high, NN)
                + mul(probe_low[...], high, NN)
                + mul(probe_high[...], low, NN)
            )
            rows = pl.ds(pl.multiple_of(number * 2 * hat_pad, 8), 2 * hat_pad)
            for part in range(length // 128):
                probe_ref[part, rows, :] = answer[:, part * 128 : (part + 1) * 128]
            return carry

        lax.fori_loop(0, depth, probe_step, 0, unroll=4)

        def green_step(number, carry):
            high, low = inverse_of(index_x * modes + number)
            answer = (
                mul(green_high_ref[...], high, NN)
                + mul(green_low_ref[...], high, NN)
                + mul(green_high_ref[...], low, NN)
            )
            green_ref[pl.ds(number, 1)] = answer[None]
            return carry

        lax.fori_loop(0, modes, green_step, 0, unroll=min(2, modes))
        here = pl.ds(pl.multiple_of(index_x * cells_a, cells_a), cells_a)
        middle = jnp.full((8, half), 0.5, F32)[0:1]
        along = cell_row_ref[0:1, :]
        point = 2.0 * cell_column_ref[here, :]
        older, newer = jnp.ones_like(point), point
        legendre_ref[0] = older
        for degree in range(1, COUNT):
            legendre_ref[degree] = newer
            older, newer = newer, (
                (2 * degree + 1) / (degree + 1) * point * newer - degree / (degree + 1) * older
            )
        for begin, count, first, second, third in (
            (0, cells_a, cell_column_ref[here, :], middle, along),
            (cells_a, cells_a, cell_column_ref[here, :], along, middle),
            (2 * cells_a, half, middle, cell_column_ref[half:, :], along),
        ):
            inverse = 1.0 / jnp.sqrt(first * first + second * second + third * third)
            unit_ref[0, begin : begin + count] = first * inverse
            unit_ref[1, begin : begin + count] = second * inverse
            unit_ref[2, begin : begin + count] = third * inverse

    field = kept(cells_a, depth, length)
    green_high, green_low = (jnp.asarray(t) for t in split_np(green))
    inputs = (
        put(eigen_column),
        put(eigen_row),
        put(lines),
        put(hat_all),
        green_high,
        green_low,
        put(cell_column),
        put(cell_row),
        sine_high,
        sine_low,
    )

    def block_of(array):
        zeros = (0,) * array.ndim
        return pl.BlockSpec(array.shape, lambda k: zeros)

    tables = call(
        prepare_body,
        (1,),
        [SCALARS] + [block_of(array) for array in inputs],
        [RESIDENT] * 8,
        [
            field,
            field,
            kept(length // 128, depth * 2 * hat_pad, 128),
            kept(modes, green.shape[0], length),
            kept(3, 2 * cells_a + half, half),
            pltpu.VMEM((2, groups_y * lanes, wide), BF16),
            pltpu.VMEM((2, length, length), BF16),
            kept(COUNT, cells_a, half),
        ],
        [
            pltpu.VMEM((depth, length), F32),
            pltpu.VMEM((2 * hat_pad, length), BF16),
            pltpu.VMEM((2 * hat_pad, length), BF16),
        ],
        10**10,
        limit=pair_limit,
    )(place, *inputs)
    edge_rows = put(np.concatenate([tabs["edges"], np.zeros((6, length))]))
    edge_columns = put(np.broadcast_to(tabs["edges"][:, :, None], (2, length, 128)))
    column_high, column_low = (jnp.asarray(t) for t in split_np(tabs["columns"]))
    lookup = np.zeros((groups_y, 24, depth))
    lookup[:, : COUNT + 2] = (
        tabs["columns"][:, : COUNT + 2].T.reshape(COUNT + 2, groups_y, depth).transpose(1, 0, 2)
    )
    lookup = lookup.reshape(groups_y, 24, blocks, block).transpose(0, 2, 1, 3)
    lookup_high, lookup_low = (jnp.asarray(t) for t in split_np(lookup))
    spread = jnp.asarray(tabs["spread"].astype(np.float32)).astype(BF16)
    factors, profile, probe_table, green_table, units, pairs, table, legendre = tables

    def second_body(*refs):
        blocks_in = refs[:groups_y]
        weights, out_ref = refs[groups_y:]
        part_tiles = out_ref.shape[0] // pack
        for start in range(0, depth, block):
            value = jnp.concatenate(
                [
                    part[:, start : start + block, :].reshape(part_tiles * block, lanes)
                    for part in blocks_in
                ],
                axis=1,
            )
            result = triple(value, weights[0], weights[1], NN) * (spacing * spacing)
            for item in range(part_tiles):
                for inner in range(pack):
                    out_ref[item * pack + inner, start : start + block, :] = result[
                        item * block : (item + 1) * block, inner * length : (inner + 1) * length
                    ]

    sources = []
    for number, parts in enumerate(received):
        sources.append(
            call(
                second_body,
                (1,),
                [RESIDENT] * (groups_y + 1),
                RESIDENT,
                kept(going[number] * pack, depth, length),
                [],
                10**9,
                limit=pair_limit,
            )(*parts, pairs)
        )

    rows_now = min(64, block)

    def solve_body(place_ref, leg_ref, *refs):
        given = refs[: len(going)]
        (
            factor_ref,
            probe_ref,
            column_high_ref,
            column_low_ref,
            lookup_high_ref,
            lookup_low_ref,
            spread_ref,
            own_ref,
            map_ref,
            mask_ref,
            field_ref,
            moment_ref,
            energy_ref,
            tensor,
        ) = refs[len(going) :]
        index_x, index_y = place_ref[0], place_ref[1]
        begin = jnp.where(index_x == 0, 1.0, 0.0)
        finish = jnp.where(index_x == groups_x - 1, 1.0, 0.0)
        step = pl.program_id(0)
        base = pl.multiple_of(step * block, block)
        window = pl.ds(base, block)

        @pl.when(step == 0)
        def _():
            tensor[...] = jnp.zeros_like(tensor)
            energy_ref[...] = jnp.zeros_like(energy_ref)

        def source(row, begin_row):
            starts = starts_of(going)
            number = max(n for n in range(len(going)) if starts[n] * pack <= row)
            return given[number][row - starts[number] * pack, pl.ds(begin_row, rows_now), :]

        def eliminate(begin_row):
            strip = pl.ds(begin_row, rows_now)
            running = source(0, begin_row) * factor_ref[0, strip, :]
            field_ref[0, strip, :] = running
            for row in range(1, cells_a):
                running = (source(row, begin_row) + running) * factor_ref[row, strip, :]
                field_ref[row, strip, :] = running
            energy = source(cells_a - 1, begin_row) * running
            for row in range(cells_a - 2, -1, -1):
                running = field_ref[row, strip, :] + factor_ref[row, strip, :] * running
                field_ref[row, strip, :] = running
                energy = energy + source(row, begin_row) * running
            energy = jnp.sum(energy.reshape(rows_now // 8, 8, length), axis=0)
            for part in range(length // 128):
                energy_ref[...] += energy[:, part * 128 : (part + 1) * 128]

        for offset in range(0, block, rows_now):
            eliminate(pl.multiple_of(base + offset, rows_now))
        first, last = field_ref[0, window, :], field_ref[cells_a - 1, window, :]
        table_high, table_low = column_high_ref[...], column_low_ref[...]
        rows_high = lookup_high_ref[index_y, step]
        rows_low = lookup_low_ref[index_y, step]

        def contract(stack, count):
            answer = triple(stack, table_high, table_low, NN)
            upper, lower = split(answer)
            outs = []
            for item in range(count):
                high = upper[item * block : (item + 1) * block]
                low = lower[item * block : (item + 1) * block]
                outs.append(
                    mul(rows_high, high, NN) + mul(rows_low, high, NN) + mul(rows_high, low, NN)
                )
            return outs

        many_rows = min(32, cells_a)
        for start in range(0, cells_a, many_rows):
            stack = field_ref[start : start + many_rows, window, :].reshape(
                many_rows * block, length
            )
            outs = contract(stack, many_rows)
            for item in range(COUNT):
                value = tensor[item]
                for inner, out in enumerate(outs):
                    value = value + leg_ref[item, start + inner : start + inner + 1, 0:128] * out
                tensor[item] = value
            if start == 0:
                tensor[COUNT] += begin * outs[0]
                tensor[COUNT + 1] -= begin * outs[0]
            if start + many_rows == cells_a:
                tensor[COUNT] += finish * outs[-1]
                tensor[COUNT + 1] += finish * outs[-1]

        def probe_row(item):
            rows = pl.ds(base * 2 * hat_pad + item, block, stride=2 * hat_pad)
            return jnp.concatenate(
                [probe_ref[part, rows, :] for part in range(length // 128)], axis=1
            )

        group = 19
        for start in range(0, functions, group):
            items = range(start, min(start + group, functions))
            stack = jnp.concatenate(
                [
                    probe_row(item) * first + probe_row(hat_pad + item) * last
                    for item in items
                ],
                axis=0,
            )
            for item, out in zip(items, contract(stack, len(items))):
                tensor[item] += out

        @pl.when(step == blocks - 1)
        def _():
            rows = lax.broadcasted_iota(jnp.int32, (8, PAIRS), 0)

            def flatten(matrix, kind):
                high, low = split(matrix)
                answer = mul(high, spread_ref[kind], NN) + mul(low, spread_ref[kind], NN)
                return jnp.sum(answer * own_ref[1 - kind], axis=0, keepdims=True)

            moments = jnp.zeros((8, TERMS), F32)
            for face in range(3):
                stack = jnp.zeros((8, PAIRS), F32)
                for parity in range(2):
                    if face == 0:
                        value = flatten(tensor[COUNT + parity], 0)
                    elif face == 1:
                        value = jnp.zeros((1, PAIRS), F32)
                        for item in range(COUNT):
                            column = tensor[item, :, COUNT + parity : COUNT + parity + 1]
                            chosen = own_ref[0, item : item + 1, :] * own_ref[1]
                            value = value + jnp.sum(column * chosen, axis=0, keepdims=True)
                    else:
                        matrix = jnp.concatenate(
                            [
                                tensor[item, COUNT + parity : COUNT + parity + 1, :]
                                for item in range(COUNT)
                            ]
                            + [jnp.zeros((24 - COUNT, 128), F32)],
                            axis=0,
                        )
                        high, low = split(matrix)
                        answer = mul(high, spread_ref[1], NN) + mul(low, spread_ref[1], NN)
                        value = jnp.sum(answer * own_ref[0], axis=0, keepdims=True)
                    stack = jnp.where(rows == parity, value, stack)
                moments = moments + exact(stack, map_ref[face], NN) * mask_ref[face]
            moments = jnp.sum(moments, axis=0, keepdims=True)
            moment_ref[...] = jnp.broadcast_to(moments[None], moment_ref.shape)

    solved, moments, energy_one = call(
        solve_body,
        (blocks,),
        [SCALARS] + [RESIDENT] * (len(going) + 11),
        [RESIDENT] * 3,
        [field, kept(devices, 1, TERMS), kept(8, 128)],
        [
            pltpu.VMEM((24, 24, 128), F32),
        ],
        10**9,
    )(
        place,
        legendre,
        *sources,
        factors,
        probe_table,
        column_high,
        column_low,
        lookup_high,
        lookup_low,
        spread,
        const("own"),
        const("maps"),
        const("masks"),
    )
    shared = lax.all_to_all(moments, ("gx", "gy"), 0, 0, tiled=True)

    folded_high, folded_low = (jnp.asarray(t) for t in split_np(tabs["folded"]))
    local_high, local_low = (
        jnp.asarray(np.ascontiguousarray(t.T).reshape(groups_y, depth, length))
        for t in split_np(tabs["folded"])
    )
    strip = min(32, cells_a)
    shares_count = block // modes
    face_rows = min(FACE_ROWS, block)

    def source_body(
        place_ref,
        share_ref,
        unit_ref,
        folded_high_ref,
        folded_low_ref,
        local_high_ref,
        local_low_ref,
        row_ref,
        column_ref,
        factor_ref,
        solved_ref,
        total_ref,
        near_ref,
        energy_ref,
        coef,
        values,
        plane_x,
        plane_y,
        plane_z,
        lines_y,
        lines_z,
        walls,
    ):
        index_x, index_y = place_ref[0], place_ref[1]
        begin = jnp.where(index_x == 0, 1.0, 0.0)
        finish = jnp.where(index_x == groups_x - 1, 1.0, 0.0)

        step = pl.program_id(0)
        window = pl.ds(pl.multiple_of(step * block, block), block)

        @pl.when(step == 0)
        def _():
            ones = jnp.full((8, 128), 0.125, F32)
            shares = jnp.broadcast_to(jnp.sum(share_ref[...], axis=0), (8, TERMS))
            coef[...] = exact(shares, ones, TN)
            energy_ref[...] = jnp.zeros_like(energy_ref)

            def one_strip(number, carry):
                window = pl.ds(pl.multiple_of(number * strip, strip), strip)
                classes = evaluate(
                    coef, unit_ref[0, window, :], unit_ref[1, window, :], unit_ref[2, window, :]
                )
                for (azimuth, kind, odd), value in classes.items():
                    values[azimuth * 4 + kind * 2 + odd, window, :] = value
                return carry

            lax.fori_loop(0, (2 * cells_a + half) // strip, one_strip, 0)
            for kind in range(2):
                for odd in range(2):
                    for start, target, row, column in (
                        (0, plane_y, kind, odd),
                        (cells_a, plane_z, odd, kind),
                    ):
                        target[
                            row * cells_a : (row + 1) * cells_a, column * half : (column + 1) * half
                        ] = (
                            values[kind * 2 + odd, start : start + cells_a, :]
                            + values[4 + kind * 2 + odd, start : start + cells_a, :]
                        )
                    even, other = (
                        values[parity * 4 + kind * 2 + odd, 2 * cells_a :, :]
                        for parity in (kind, 1 - kind)
                    )
                    plane_x[
                        kind * half : (kind + 1) * half, odd * half : (odd + 1) * half
                    ] = even + (finish - begin) * other
            folded_tables = folded_high_ref[...], folded_low_ref[...]
            local_tables = local_high_ref[index_y], local_low_ref[index_y]

            def across(plane):
                upper, lower = split(plane)
                high, low = local_tables
                return mul(high, upper, NT) + mul(low, upper, NT) + mul(high, lower, NT)

            lines_z[...] = triple(plane_z[...], *folded_tables, NN)
            lines_y[...] = across(plane_y[...])
            wall = triple(across(plane_x[...]), *folded_tables, NN)
            walls[0] = begin * wall
            walls[1] = finish * wall


        def eliminate(offset):
            begin_row = pl.multiple_of(step * block + offset, face_rows)
            window = pl.ds(begin_row, face_rows)
            here = pl.ds(pl.multiple_of(index_y * depth + begin_row, face_rows), face_rows)
            columns = [
                jnp.concatenate([column_ref[parity, here, :]] * (length // 128), axis=1)
                for parity in range(2)
            ]
            line_block = lines_y[window, :]
            energy = jnp.zeros((face_rows, length), F32)
            running = None
            for row in range(cells_a):
                value = None
                for parity in range(2):
                    spot = parity * cells_a + row
                    term = line_block[:, spot : spot + 1] * row_ref[parity : parity + 1, :]
                    value = term if value is None else value + term
                    value = value + lines_z[spot : spot + 1, :] * columns[parity]
                if row == 0:
                    value = value + walls[0, window, :]
                if row == cells_a - 1:
                    value = value + walls[1, window, :]
                energy = energy + value * solved_ref[row, window, :]
                running = value if running is None else value + running
                running = running * factor_ref[row, window, :]
                total_ref[row, window, :] = running
            nears = [solved_ref[0, window, :], solved_ref[cells_a - 1, window, :], None, running]
            total_ref[cells_a - 1, window, :] = nears[1] + running
            for row in range(cells_a - 2, -1, -1):
                running = total_ref[row, window, :] + factor_ref[row, window, :] * running
                total_ref[row, window, :] = solved_ref[row, window, :] + running
            nears[2] = running
            for item in range(face_rows // modes):
                for number, value in enumerate(nears):
                    near_ref[(step * block + offset) // modes + item, number] = value[
                        item * modes : (item + 1) * modes
                    ]
            energy = jnp.sum(energy.reshape(face_rows // 8, 8, length), axis=0)
            for part in range(length // 128):
                energy_ref[...] += energy[:, part * 128 : (part + 1) * 128]

        for offset in range(0, block, face_rows):
            eliminate(offset)

    total, nears, energy_two = call(
        source_body,
        (blocks,),
        [SCALARS] + [RESIDENT] * 10,
        [RESIDENT] * 3,
        [field, kept(groups_x, 4, modes, length), kept(8, 128)],
        [
            pltpu.VMEM((TERMS, 128), F32),
            kept(8, 2 * cells_a + half, half),
            pltpu.VMEM((length, length), F32),
            pltpu.VMEM((2 * cells_a, length), F32),
            pltpu.VMEM((2 * cells_a, length), F32),
            pltpu.VMEM((depth, 2 * cells_a), F32),
            pltpu.VMEM((2 * cells_a, length), F32),
            pltpu.VMEM((2, depth, length), F32),
        ],
        10**9,
    )(
        place,
        shared,
        units,
        folded_high,
        folded_low,
        local_high,
        local_low,
        edge_rows,
        edge_columns,
        factors,
        solved,
    )

    gathered = lax.all_to_all(nears, "gx", 0, 0, tiled=True)

    def ghost_body(near_ref, green_ref, one_ref, two_ref, out_ref):
        first = [near_ref[s, 0] for s in range(groups_x)]
        last = [near_ref[s, 1] for s in range(groups_x)]
        other_first = [near_ref[s, 2] for s in range(groups_x)]
        other_last = [near_ref[s, 3] for s in range(groups_x)]
        energy_one = jnp.zeros((modes, length), F32)
        energy_two = jnp.zeros((modes, length), F32)
        for slab in range(groups_x):
            for side in range(2):
                value = jnp.zeros((modes, length), F32)
                other = jnp.zeros((modes, length), F32)
                neighbour = slab + (1 if side else -1)
                if 0 <= neighbour < groups_x:
                    value = (first if side else last)[neighbour]
                    other = (other_first if side else other_last)[neighbour]
                    for s in range(groups_x):
                        for end, one, two in (
                            (0, first, other_first),
                            (1, last, other_last),
                        ):
                            row = green_row.get((2 * slab + side, 2 * s + end))
                            if row is not None:
                                green = green_ref[:, row, :]
                                value = value + green * one[s]
                                other = other + green * two[s]
                energy_one = energy_one + value * (last if side else first)[slab]
                energy_two = energy_two + value * (other_last if side else other_first)[slab]
                out_ref[slab, side * modes : (side + 1) * modes, :] = value + other
        top = lax.broadcasted_iota(jnp.int32, (8, 128), 0) == 0
        for number, (local_ref, value) in enumerate(((one_ref, energy_one), (two_ref, energy_two))):
            value = jnp.sum(value, axis=0, keepdims=True)
            line = value[:, 0:128]
            for part in range(1, length // 128):
                line = line + value[:, part * 128 : (part + 1) * 128]
            tile = local_ref[...] + jnp.where(top, line, 0.0)
            for slab in range(groups_x):
                out_ref[slab, 2 * modes : 2 * modes + 8, number * 128 : (number + 1) * 128] = tile

    height = 2 * modes + 8
    answers = call(
        ghost_body, (1,), [RESIDENT] * 4, RESIDENT, kept(groups_x, height, length), [], 10**8
    )(gathered, green_table, energy_one, energy_two)
    returned = lax.all_to_all(answers, "gx", 0, 0, tiled=True)

    def back_body(number, total_ref, profile_ref, ghost_ref, weights, *rest):
        outs, energy_ref = rest[:groups_y], rest[groups_y]
        energy_ref[...] = jnp.sum(ghost_ref[:, 2 * modes : 2 * modes + 8, 0:256], axis=0)
        for step in range(blocks):
            back_block(total_ref, profile_ref, ghost_ref, outs, weights, step, number)

    def back_block(total_ref, profile_ref, ghost_ref, outs, weights, step, number):
        window = pl.ds(step * block, block)
        ghosts_here = [
            jnp.concatenate(
                [
                    ghost_ref[step * shares_count + item, side * modes : (side + 1) * modes, :]
                    for item in range(shares_count)
                ],
                axis=0,
            )
            for side in range(2)
        ]

        parts = []
        for item in range(starts_of(coming)[number], starts_of(coming)[number] + coming[number]):
            inner = []
            for row in range(item * pack, (item + 1) * pack):
                inner.append(
                    total_ref[row, window, :]
                    + profile_ref[row, window, :] * ghosts_here[0]
                    + profile_ref[cells_a - 1 - row, window, :] * ghosts_here[1]
                )
            parts.append(jnp.concatenate(inner, axis=1))
        result = triple(jnp.concatenate(parts, axis=0), weights[0], weights[1], NT)
        for shift in range(groups_y):
            for item in range(coming[number]):
                outs[shift][item, window, :] = result[
                    item * block : (item + 1) * block, shift * lanes : (shift + 1) * lanes
                ]

    arrived = []
    for number in range(len(coming)):
        *parts, tile_now = call(
            functools.partial(back_body, number),
            (1,),
            [RESIDENT] * 4,
            [RESIDENT] * (groups_y + 1),
            pieces_of(coming[number]) + [kept(8, 256)],
            [],
            10**9,
            limit=pair_limit,
        )(total, profile, returned, pairs)
        energy_tile = tile_now if number == 0 else energy_tile
        arrived.append(exchange(parts))
    energy_tiles = exchange([energy_tile] * groups_y)

    norm = (2.0 / (length + 1)) ** 2

    def last_body(*refs):
        blocks_in = refs[:groups_y]
        table, out_ref = refs[groups_y], refs[-1]
        start = pl.program_id(0) * many
        values = [
            jnp.concatenate([part[start + item] for part in blocks_in], axis=0).T
            for item in range(many)
        ]
        result = triple(jnp.concatenate(values, axis=0), table[0], table[1], NN) * norm
        out_ref[...] = result.reshape(many * pack, cells_b, length)

    def final_body(*refs):
        tiles_in = refs[-2 - groups_y : -2]
        energy_ref = refs[-1]
        last_body(*refs[: groups_y + 1], refs[-2])

        @pl.when(pl.program_id(0) == 0)
        def _():
            value = tiles_in[0][...]
            for tile in tiles_in[1:]:
                value = value + tile[...]
            factor = spacing * norm
            first = jnp.sum(value[:, 0:128]) * factor
            energy_ref[0] = first
            energy_ref[1] = first + jnp.sum(value[:, 128:256]) * factor

    shape = jax.ShapeDtypeStruct(charge_density.shape, F32)
    base_specs = [RESIDENT] * (groups_y + 1)
    out_block = (many * pack, cells_b, length)
    potential = None
    for number in range(len(coming)):
        steps, first = coming[number] // many, starts_of(coming)[number] // many
        inputs = [*arrived[number], table]
        specs, aliases = list(base_specs), None
        if number > 0:
            aliases = {len(inputs): 0}
            inputs.append(potential)
            specs.append(pl.BlockSpec(memory_space=pl.ANY))
        out_spec = pl.BlockSpec(out_block, lambda t, first=first: (t + first, 0, 0))
        if number < len(coming) - 1:
            potential = call(
                last_body, (steps,), specs, out_spec, shape, [], 10**9, aliases
            )(*inputs)
        else:
            potential, energies = call(
                final_body,
                (steps,),
                specs + [RESIDENT] * groups_y,
                [out_spec, SCALARS],
                [shape, jax.ShapeDtypeStruct((2,), F32)],
                [],
                10**9,
                aliases,
            )(*inputs, *energy_tiles)
    return potential, energies


def solution(mesh):
    placed = (P("gx", "gy", None),)
    return jax.shard_map(
        shards, mesh=mesh, in_specs=placed, out_specs=(P("gx", "gy", None), P()), check_vma=False
    )
```
